32 devices in a mesh: row: 8 (over z, x), col: 4 (over y, core).
Axes of the slice: x: 2, y: 2, z: 4, core: 2. Of those that a mesh axis runs over, the one named last changes fastest.
Arguments:
- tile_values: bfloat16 [192, 512, 128], P('row', 'col'), may hold values from -0.0546875 to 0.0546875
- tile_counts: int32 [96, 4], P('row', 'col'), may hold values from 0 to 2, as said below
- tile_cols: int32 [192, 4], P('row', 'col'), may hold values from 0 to 1, as said below
- panels: bfloat16 [12288, 4096], P('row', 'col'), may hold values from -6 to 6
Outputs:
- product: bfloat16 [1024, 4096], P('col', 'row')
The draws below stay inside these ranges and needn't reach their ends.
Inputs may be any that keep to these rules, and one draw needn't show every extreme that they name: `tile_counts`: within each device the filled slots follow block row order; a device holds at most 24 tiles and some device holds exactly 24 in every draw. `tile_cols`: within one block row of a device the filled slots' columns rise strictly; entries of unfilled slots carry no meaning.
All inputs are finite; a program needn't handle non-finite values.
Results may differ from the reference program's by a relative error of at most 0.001.
Values may be sent and summed in bfloat16 or wider, within the bound.
A program may use at most 64 MiB of HBM per device.

```python
import jax
import jax.numpy as jnp
from jax import lax

TILE = 128
NB = 4096
BR_DEV = 12
BC_DEV = 2
CAP = 24
ROWS = 12288
COLS = 1024
N_ROW = 8
N_COL = 4


def tile_pattern(key):
    base = jax.random.fold_in(key, 7)
    key_levels = jax.random.fold_in(base, 1)
    key_rolled = jax.random.fold_in(base, 2)
    key_chosen = jax.random.fold_in(base, 3)
    levels = jax.random.randint(key_levels, (N_ROW, N_COL, BR_DEV, 1), 0, 5)
    chosen = jax.random.randint(key_chosen, (), 0, N_ROW * N_COL)
    device_ids = jnp.arange(N_ROW, dtype=jnp.int32)[:, None] * N_COL + jnp.arange(N_COL, dtype=jnp.int32)[None, :]
    levels = jnp.where((device_ids == chosen)[:, :, None, None], 4, levels)
    rolled = jax.random.randint(key_rolled, (N_ROW, N_COL, BR_DEV, BC_DEV), 0, 4)
    present = (rolled < levels).astype(jnp.int32)
    counts = jnp.sum(present, axis=-1).astype(jnp.int32)
    row_start = (jnp.cumsum(counts, axis=-1) - counts).astype(jnp.int32)
    within = (jnp.cumsum(present, axis=-1) - present).astype(jnp.int32)
    slot_index = jnp.where(present == 1, row_start[..., None] + within, CAP).astype(jnp.int32)
    col_index = jnp.broadcast_to(jnp.arange(BC_DEV, dtype=jnp.int32), present.shape)

    def place_row(slots, values):
        return jnp.zeros((CAP,), jnp.int32).at[slots].set(values, mode='drop')
    columns = jax.vmap(place_row)(slot_index.reshape(N_ROW * N_COL, BR_DEV * BC_DEV), col_index.reshape(N_ROW * N_COL, BR_DEV * BC_DEV))
    return (counts, columns.reshape(N_ROW, N_COL, CAP))


def draw_tile_counts(key, part):
    counts, columns = tile_pattern(key)
    return jnp.transpose(counts, (0, 2, 1)).reshape(N_ROW * BR_DEV, N_COL)


def draw_tile_cols(key, part):
    counts, columns = tile_pattern(key)
    return jnp.transpose(columns, (0, 2, 1)).reshape(N_ROW * CAP, N_COL)


def strengthened(array, stream_key, source, target, blocks, factor):
    owner, partner = [(jnp.arange(array.shape[dim]) // (array.shape[dim] // blocks)).reshape([-1 if axis == dim else 1 for axis in range(array.ndim)]) for dim in (source, target)]
    chosen = jax.random.permutation(stream_key, blocks)[partner]
    strong = (owner == chosen) | (owner == (partner + blocks // 2) % blocks)
    return jnp.where(strong, factor * array, array)


def block_levels(stream_key, dims, split, smallest, top_value):
    factor_of, own = 1.0, jax.random.fold_in(stream_key, 6)
    for axis_at, blocks in split:
        steps = jnp.exp(jax.random.uniform(jax.random.fold_in(own, axis_at), (blocks,), jnp.float32, smallest / len(split), top_value / len(split)))
        factor_of = factor_of * jnp.repeat(steps, dims[axis_at] // blocks).reshape([-1 if axis == axis_at else 1 for axis in range(len(dims))])
    return factor_of


def centred(stream_key, dims, width, reach, cuts=(), kind=jnp.bfloat16):
    entries = width * jax.random.normal(stream_key, dims, jnp.float32)
    if cuts:
        entries = entries * block_levels(stream_key, dims, cuts, -0.22, 0.18)
    return jnp.clip(entries, -reach, reach).astype(kind)


def noise_with(key, shape, width, reach, shards, heavy, held_as=jnp.bfloat16):
    drawn = width * jax.random.normal(key, shape, jnp.float32)
    if shards:
        drawn = drawn * block_levels(key, shape, shards, -0.22, 0.18)
    return jnp.clip(strengthened(drawn, jax.random.fold_in(key, 3), *heavy), -reach, reach).astype(held_as)


def setup_inputs(seed: int = 0) -> dict:
    key_of = jax.random.split(jax.random.key(seed), 5)
    return {
        "tile_values": centred(key_of[0], (N_ROW * CAP, N_COL * TILE, TILE), (TILE * BR_DEV * N_ROW) ** -0.5, 0.0546875, ((0, 8), (1, 4))),
        "tile_counts": draw_tile_counts(jax.random.fold_in(key_of[4], 71), 0),
        "tile_cols": draw_tile_cols(jax.random.fold_in(key_of[4], 71), 0),
        "panels": noise_with(key_of[3], (ROWS, NB), 1.0, 6.0, ((0, 8), (1, 4)), (0, 1, 8, 2.0)),
    }


def reference(tile_values, tile_counts, tile_cols, panels):
    def add_group(row_dev, totals):
        row_dev = jnp.asarray(row_dev).astype(jnp.int32)
        tile_slab = lax.dynamic_slice_in_dim(tile_values, row_dev * CAP, CAP, 0)
        tile_slab = tile_slab.astype(jnp.float32).reshape(CAP, N_COL, TILE, TILE)
        counts = lax.dynamic_slice_in_dim(tile_counts, row_dev * BR_DEV, BR_DEV, 0).astype(jnp.int32)
        columns = lax.dynamic_slice_in_dim(tile_cols, row_dev * CAP, CAP, 0).astype(jnp.int32)
        row_start = (jnp.cumsum(counts, axis=0) - counts).astype(jnp.int32)
        slot_ids = jnp.arange(CAP, dtype=jnp.int32)[:, None, None]
        row_mask = ((slot_ids >= row_start[None]) & (slot_ids < (row_start + counts)[None])).astype(jnp.float32)
        col_mask = (columns[:, None, :] == jnp.arange(BC_DEV, dtype=jnp.int32)[None, :, None]).astype(jnp.float32)
        dense_rows = jnp.einsum("sic,sjc,scab->iacjb", row_mask, col_mask, tile_slab)
        dense_rows = dense_rows.reshape(BR_DEV * TILE, N_COL * BC_DEV * TILE).astype(jnp.bfloat16)
        panel_rows = lax.dynamic_slice_in_dim(panels, row_dev * BR_DEV * TILE, BR_DEV * TILE, 0)
        return totals + lax.dot_general(dense_rows, panel_rows, (((0,), (0,)), ((), ())), preferred_element_type=jnp.float32)

    totals = lax.fori_loop(0, N_ROW, add_group, jnp.zeros((COLS, NB), jnp.float32))
    return totals.astype(jnp.bfloat16)
```

```python
import functools

import jax
import jax.numpy as jnp
from jax import lax
from jax.experimental import pallas as pl
from jax.experimental.pallas import tpu as pltpu
from jax.sharding import PartitionSpec as P

BC_DEV = 2
PAIR = 2
SUB = 2
LAG_OUTER = 2
LAG_INNER = 5
LAG_FINAL = 8
TOP = 32767.0
MESH = pl.DeviceIdType.MESH
SELF, SIDE, FAR, FAR_SIDE = range(4)


def chunk_order(n_y):
    pieces = BC_DEV * SUB
    near = [(SELF, 0, p) for p in range(pieces)] + [(SIDE, 0, p) for p in range(pieces)]
    order, near = near[: pieces + 1], near[pieces + 1 :]
    for p in range(pieces):
        for dy in range(1, n_y):
            order += [(FAR, dy, p), (FAR_SIDE, dy, p)]
            if len(near) > 1:
                order.append(near.pop(0))
    return order + near


def pick(i, values):
    out = jnp.int32(values[0])
    for t, v in enumerate(values):
        if v != values[0]:
            out = jnp.where(i == t, jnp.int32(v), out)
    return out


def encode(value, code_ref, step_ref):
    peak = jnp.maximum(jnp.max(jnp.abs(value), axis=0, keepdims=True), 1e-30)
    code_ref[...] = jnp.round(value * (TOP / peak)).astype(jnp.int32).astype(jnp.int16)
    step_ref[...] = peak * (1.0 / TOP)


def decode(code_ref, step_ref):
    return code_ref[...].astype(jnp.int32).astype(jnp.float32) * step_ref[...]


def build_dense(j, counts_ref, cols_ref, tiles_ref, at_ref):
    slots, tile, _ = tiles_ref.shape
    half = tile // SUB
    start = jnp.int32(0)
    for i in range(counts_ref.shape[1]):
        count = counts_ref[0, i]
        here = jnp.minimum(start, slots - 1)
        after = jnp.minimum(start + 1, slots - 1)
        one = (count > 0) & (cols_ref[0, here] == j)
        two = (count > 1) & (cols_ref[0, after] == j)
        block = tiles_ref[jnp.where(two, after, here)]
        keep = jnp.where(one | two, 1.0, 0.0).astype(jnp.float32)
        block = (block.astype(jnp.float32) * keep).T.astype(jnp.bfloat16)
        for h in range(SUB):
            at_ref[SUB * j + h, :, i * tile : (i + 1) * tile] = block[h * half : (h + 1) * half]
        start = start + count


def kernel(
    n_row, n_col, counts_ref, cols_ref, tiles_hbm, b_hbm, o_ref,
    tiles_ref, b_away, b_own, at_ref, total_ref, own_ref, xs, xr, zs, zup, zdn, zsk,
    fin_ref, land_ref, load_sem,
    at_send, at_recv, fw_send, x_send, x_recv, z_send, up_recv, dn_recv, sk_recv, f_send, f_recv,
):
    row, col = lax.axis_index("row"), lax.axis_index("col")
    n_z, n_y = n_row // PAIR, n_col // PAIR
    order = chunk_order(n_y)
    chunks, pieces = len(order), BC_DEV * SUB
    z, x = row // PAIR, lax.rem(row, PAIR)
    y, k = col // PAIR, lax.rem(col, PAIR)
    wide = b_own.shape[1]
    place = {c: i for i, c in enumerate(order)}

    def row_of(z_at, x_at):
        return z_at * PAIR + x_at

    def col_of(y_at, k_at):
        return y_at * PAIR + k_at

    def load(src, dst, i):
        return pltpu.make_async_copy(src, dst, load_sem.at[i])

    at_away = pl.ds(pl.multiple_of((1 - x) * wide, wide), wide)
    at_own = pl.ds(pl.multiple_of(x * wide, wide), wide)
    loads = [
        load(tiles_hbm, tiles_ref, 0),
        load(b_hbm.at[:, at_away], b_away, 1),
        load(b_hbm.at[:, at_own], b_own, 2),
    ]
    for c in loads:
        c.start()

    beside = (row_of(z, 1 - x), col)
    partner = (row, col_of(y, 1 - k))
    final = z == col
    even = k == 0
    skip_up = even & (z == col + 2)
    skip_dn = jnp.logical_not(even) & (z == col - 2)
    skips = skip_up | skip_dn
    goes_down = (z > col) & jnp.logical_not(skip_up)
    goes_up = (z < col) & jnp.logical_not(skip_dn)
    from_above = (z >= col) & (z < n_z - 1) & jnp.logical_not(even & (z == col + 1))
    from_below = (z <= col) & (z > 0) & jnp.logical_not(jnp.logical_not(even) & (z == col - 1))
    from_skip = final & ((even & (col + 2 < n_z)) | (jnp.logical_not(even) & (col >= 2)))
    above = (row_of(jnp.minimum(z + 1, n_z - 1), x), col)
    below = (row_of(jnp.maximum(z - 1, 0), x), col)
    skip_to = (row_of(jnp.minimum(col, n_z - 1), x), col)
    skip_of = (row_of(jnp.clip(jnp.where(even, col + 2, col - 2), 0, n_z - 1), x), col)

    def flag(b):
        return jnp.where(b, 1, 0).astype(jnp.int32)

    barrier = pltpu.get_barrier_semaphore()

    def greet(device):
        pl.semaphore_signal(barrier, inc=1, device_id=device, device_id_type=MESH)

    greet(beside)
    for step in range(1, n_col):
        greet((row, lax.rem(col + step, n_col)))
    pl.when(z < n_z - 1)(lambda: greet(above))
    pl.when(z > 0)(lambda: greet(below))
    pl.when(skips)(lambda: greet(skip_to))
    pl.when(from_skip)(lambda: greet(skip_of))

    def copy(src, dst, send, recv, device):
        return pltpu.make_async_remote_copy(
            src_ref=src, dst_ref=dst, send_sem=send, recv_sem=recv,
            device_id=device, device_id_type=MESH,
        )

    loads[0].wait()
    first = []
    for j in range(BC_DEV):
        build_dense(j, counts_ref, cols_ref, tiles_ref, at_ref)
        if j == 0:
            pl.semaphore_wait(
                barrier, n_col + flag(z < n_z - 1) + flag(z > 0) + flag(skips) + flag(from_skip)
            )
        for p in range(j * SUB, (j + 1) * SUB):
            here = place[(SELF, 0, p)]
            assert here == p
            for dy in range(1, n_y):
                to = (row, col_of(lax.rem(y + n_y - dy, n_y), k))
                there = place[(FAR, dy, p)]
                first.append(copy(at_ref.at[here], at_ref.at[there], at_send.at[dy * pieces + p],
                                  at_recv.at[there], to))
                first[-1].start()
            there = place[(SIDE, 0, p)]
            first.append(copy(at_ref.at[here], at_ref.at[there], at_send.at[p],
                              at_recv.at[there], partner))
            first[-1].start()

    kinds, dys, ps = ([c[t] for c in order] for t in range(3))

    def forward(i):
        return copy(at_ref.at[i], at_ref.at[i + 1], fw_send.at[i], at_recv.at[i + 1], partner)

    class Both:
        def __init__(self, src, dst, send, recv, i, device):
            self.parts = [
                copy(src[t].at[i], dst[t].at[i], send.at[t, i], recv.at[t, i], device)
                for t in range(2)
            ]

        def start(self):
            for part in self.parts:
                part.start()

        def wait_send(self):
            for part in self.parts:
                part.wait_send()

        def wait_recv(self):
            for part in self.parts:
                part.wait_recv()

    def x_copy(i):
        return Both(xs, xr, x_send, x_recv, i, beside)

    def down_copy(i):
        return Both(zs, zup, z_send, up_recv, i, below)

    def up_copy(i):
        return Both(zs, zdn, z_send, dn_recv, i, above)

    def skip_copy(i):
        return Both(zs, zsk, z_send, sk_recv, i, skip_to)

    def fin_copy(i):
        kind, dy, p = pick(i, kinds), pick(i, dys), pick(i, ps)
        odd = lax.rem(kind, 2)
        to = (row, col_of(lax.rem(y + dy, n_y), lax.rem(k + odd, PAIR)))
        return copy(fin_ref.at[i], land_ref.at[p], f_send.at[i], f_recv.at[p], to)

    def compute(i):
        kind = pick(i, kinds)

        @pl.when(kind != SELF)
        def _():
            copy(at_ref.at[i], at_ref.at[i], fw_send.at[i], at_recv.at[i], partner).wait_recv()

        @pl.when(kind == FAR)
        def _():
            forward(i).start()

        lhs = at_ref[i]
        encode(jnp.dot(lhs, b_away[...], preferred_element_type=jnp.float32), xs[0].at[i], xs[1].at[i])
        x_copy(i).start()
        own_ref[i] = jnp.dot(lhs, b_own[...], preferred_element_type=jnp.float32)

    def combine(i):
        x_copy(i).wait_recv()
        total_ref[...] = own_ref[i] + decode(xr[0].at[i], xr[1].at[i])

        @pl.when(from_above)
        def _():
            down_copy(i).wait_recv()
            total_ref[...] += decode(zup[0].at[i], zup[1].at[i])

        @pl.when(from_below)
        def _():
            up_copy(i).wait_recv()
            total_ref[...] += decode(zdn[0].at[i], zdn[1].at[i])

        @pl.when(from_skip)
        def _():
            skip_copy(i).wait_recv()
            total_ref[...] += decode(zsk[0].at[i], zsk[1].at[i])

        @pl.when(jnp.logical_not(final))
        def _():
            encode(total_ref[...], zs[0].at[i], zs[1].at[i])

        @pl.when(goes_down)
        def _():
            down_copy(i).start()

        @pl.when(goes_up)
        def _():
            up_copy(i).start()

        @pl.when(skips)
        def _():
            skip_copy(i).start()

        @pl.when(final)
        def _():
            fin_ref[i] = total_ref[...].astype(jnp.bfloat16)

            @pl.when(pick(i, kinds) != SELF)
            def _():
                fin_copy(i).start()

    inner = jnp.logical_not(final) & (from_above | from_below)
    lag = jnp.where(final, LAG_FINAL, jnp.where(inner, LAG_INNER, LAG_OUTER))

    loads[1].wait()
    loads[2].wait()

    def main(i, carry):
        @pl.when(i < chunks)
        def _():
            compute(i)

        @pl.when((i >= lag) & (i < chunks + lag))
        def _():
            combine(i - lag)

        return carry

    lax.fori_loop(0, chunks + LAG_FINAL, main, 0)

    rows = land_ref.shape[1]
    for p in range(pieces):
        @pl.when(final)
        def _(p=p):
            o_ref[p * rows : (p + 1) * rows] = fin_ref[p]

        @pl.when(jnp.logical_not(final))
        def _(p=p):
            copy(fin_ref.at[p], land_ref.at[p], f_send.at[p], f_recv.at[p], partner).wait_recv()
            o_ref[p * rows : (p + 1) * rows] = land_ref[p]

    for c in first:
        c.wait_send()

    def drain(i, carry):
        x_copy(i).wait_send()

        @pl.when(pick(i, kinds) == FAR)
        def _():
            forward(i).wait_send()

        @pl.when(jnp.logical_not(final))
        def _():
            down_copy(i).wait_send()

        @pl.when(final & (pick(i, kinds) != SELF))
        def _():
            fin_copy(i).wait_send()

        return carry

    lax.fori_loop(0, chunks, drain, 0)


def per_device(n_row, n_col, tile_values, tile_counts, tile_cols, panels):
    slots, tile, _ = tile_values.shape
    deep, columns = panels.shape
    wide = columns // PAIR
    pieces = BC_DEV * SUB
    chunks = pieces * n_col
    rows = tile // SUB
    f32, bf16 = jnp.float32, jnp.bfloat16
    vmem = pl.BlockSpec(memory_space=pltpu.VMEM)
    smem = pl.BlockSpec(memory_space=pltpu.SMEM)
    hbm = pl.BlockSpec(memory_space=pl.ANY)
    dma = pltpu.SemaphoreType.DMA
    coded = (pltpu.VMEM((chunks, rows, wide), jnp.int16), pltpu.VMEM((chunks, 1, wide), f32))
    return pl.pallas_call(
        functools.partial(kernel, n_row, n_col),
        out_shape=jax.ShapeDtypeStruct((BC_DEV * tile, wide), bf16),
        in_specs=[smem, smem, hbm, hbm],
        out_specs=vmem,
        scratch_shapes=[
            pltpu.VMEM((slots, tile, tile), bf16),
            pltpu.VMEM((deep, wide), bf16),
            pltpu.VMEM((deep, wide), bf16),
            pltpu.VMEM((chunks, rows, deep), bf16),
            pltpu.VMEM((rows, wide), f32),
            pltpu.VMEM((chunks, rows, wide), f32),
            coded,
            coded,
            coded,
            coded,
            coded,
            coded,
            pltpu.VMEM((chunks, rows, wide), bf16),
            pltpu.VMEM((pieces, rows, wide), bf16),
            dma((3,)),
            dma((n_col // PAIR * pieces,)),
            dma((chunks,)),
            dma((chunks,)),
            dma((2, chunks)),
            dma((2, chunks)),
            dma((2, chunks)),
            dma((2, chunks)),
            dma((2, chunks)),
            dma((2, chunks)),
            dma((chunks,)),
            dma((pieces,)),
        ],
        compiler_params=pltpu.CompilerParams(
            collective_id=0, has_side_effects=True, vmem_limit_bytes=56 * 1024 * 1024
        ),
    )(tile_counts.T, tile_cols.T, tile_values, panels)


def solution(mesh):
    n_row, n_col = mesh.shape["row"], mesh.shape["col"]
    return jax.shard_map(
        functools.partial(per_device, n_row, n_col),
        mesh=mesh,
        in_specs=(P("row", "col", None), P("row", "col"), P("row", "col"), P("row", "col")),
        out_specs=P("col", "row"),
        check_vma=False,
    )
```

```python
import functools

import jax
import jax.numpy as jnp
from jax import lax
from jax.experimental import pallas as pl
from jax.experimental.pallas import tpu as pltpu
from jax.sharding import PartitionSpec as P

BC_DEV = 2
PAIR = 2
SUB = 2
LAG_OUTER = 2
LAG_INNER = 5
LAG_FINAL = 8
TOP = 32767.0
MESH = pl.DeviceIdType.MESH
SELF, SIDE, FAR, FAR_SIDE = range(4)


def chunk_order(n_y):
    pieces = BC_DEV * SUB
    near = [(SELF, 0, p) for p in range(pieces)] + [(SIDE, 0, p) for p in range(pieces)]
    order, near = near[: pieces + 1], near[pieces + 1 :]
    for p in range(pieces):
        for dy in range(1, n_y):
            order += [(FAR, dy, p), (FAR_SIDE, dy, p)]
            if len(near) > 1:
                order.append(near.pop(0))
    return order + near


def pick(i, values):
    out = jnp.int32(values[0])
    for t, v in enumerate(values):
        if v != values[0]:
            out = jnp.where(i == t, jnp.int32(v), out)
    return out


def encode(value, code_ref, step_ref):
    peak = jnp.maximum(jnp.max(jnp.abs(value), axis=0, keepdims=True), 1e-30)
    code_ref[...] = jnp.round(value * (TOP / peak)).astype(jnp.int32).astype(jnp.int16)
    step_ref[...] = peak * (1.0 / TOP)


def decode(code_ref, step_ref):
    return code_ref[...].astype(jnp.int32).astype(jnp.float32) * step_ref[...]


def build_dense(j, counts_ref, cols_ref, tiles_ref, at_ref):
    slots, tile, _ = tiles_ref.shape
    half = tile // SUB
    start = jnp.int32(0)
    for i in range(counts_ref.shape[1]):
        count = counts_ref[0, i]
        here = jnp.minimum(start, slots - 1)
        after = jnp.minimum(start + 1, slots - 1)
        one = (count > 0) & (cols_ref[0, here] == j)
        two = (count > 1) & (cols_ref[0, after] == j)
        block = tiles_ref[jnp.where(two, after, here)]
        keep = jnp.where(one | two, 1.0, 0.0).astype(jnp.float32)
        block = (block.astype(jnp.float32) * keep).T.astype(jnp.bfloat16)
        for h in range(SUB):
            at_ref[SUB * j + h, :, i * tile : (i + 1) * tile] = block[h * half : (h + 1) * half]
        start = start + count


def kernel(
    n_row, n_col, counts_ref, cols_ref, tiles_hbm, b_hbm, o_ref,
    tiles_ref, b_away, b_own, at_ref, total_ref, own_ref, xs, xr, zs, zup, zdn,
    fin_ref, land_ref, size_ref, load_sem,
    at_send, at_recv, fw_send, x_send, x_recv, z_send, up_recv, dn_recv, f_send, f_recv, out_sem,
):
    row, col = lax.axis_index("row"), lax.axis_index("col")
    n_z, n_y = n_row // PAIR, n_col // PAIR
    order = chunk_order(n_y)
    chunks, pieces = len(order), BC_DEV * SUB
    z, x = row // PAIR, lax.rem(row, PAIR)
    y, k = col // PAIR, lax.rem(col, PAIR)
    wide = b_own.shape[1]
    place = {c: i for i, c in enumerate(order)}

    def row_of(z_at, x_at):
        return z_at * PAIR + x_at

    def col_of(y_at, k_at):
        return y_at * PAIR + k_at

    def load(src, dst, i):
        return pltpu.make_async_copy(src, dst, load_sem.at[i])

    at_away = pl.ds(pl.multiple_of((1 - x) * wide, wide), wide)
    at_own = pl.ds(pl.multiple_of(x * wide, wide), wide)
    loads = [
        load(tiles_hbm, tiles_ref, 0),
        load(b_hbm.at[:, at_away], b_away, 1),
        load(b_hbm.at[:, at_own], b_own, 2),
    ]
    for c in loads:
        c.start()

    beside = (row_of(z, 1 - x), col)
    partner = (row, col_of(y, 1 - k))
    final = z == col
    skip_up = (col == 0) & (z == 2)
    skip_dn = (col == n_z - 1) & (z == n_z - 3)
    skips = skip_up | skip_dn
    goes_down = (z > col) & jnp.logical_not(skip_up)
    goes_up = (z < col) & jnp.logical_not(skip_dn)
    low_end, high_end = (z == 0) & (col == 0), (z == n_z - 1) & (col == n_z - 1)
    from_above = (z >= col) & (z < n_z - 1) & jnp.logical_not((col == 0) & (z == 1)) | high_end
    from_below = (z <= col) & (z > 0) & jnp.logical_not((col == n_z - 1) & (z == n_z - 2)) | low_end
    from_skip = low_end | high_end
    above = (row_of(jnp.minimum(z + 1, n_z - 1), x), col)
    below = (row_of(jnp.maximum(z - 1, 0), x), col)
    skip_to = (row_of(jnp.minimum(col, n_z - 1), x), col)
    skip_of = (row_of(jnp.where(low_end, 2, n_z - 3), x), col)

    def flag(b):
        return jnp.where(b, 1, 0).astype(jnp.int32)

    barrier = pltpu.get_barrier_semaphore()

    def greet(device):
        pl.semaphore_signal(barrier, inc=1, device_id=device, device_id_type=MESH)

    greet(beside)
    for step in range(1, n_col):
        greet((row, lax.rem(col + step, n_col)))
    pl.when(z < n_z - 1)(lambda: greet(above))
    pl.when(z > 0)(lambda: greet(below))
    pl.when(skips)(lambda: greet(skip_to))
    pl.when(from_skip)(lambda: greet(skip_of))

    def copy(src, dst, send, recv, device):
        return pltpu.make_async_remote_copy(
            src_ref=src, dst_ref=dst, send_sem=send, recv_sem=recv,
            device_id=device, device_id_type=MESH,
        )

    with jax.named_scope("wait_tiles"):
        loads[0].wait()
    first = []
    for j in range(BC_DEV):
        with jax.named_scope("build"):
            build_dense(j, counts_ref, cols_ref, tiles_ref, at_ref)
        if j == 0:
            with jax.named_scope("wait_barrier"):
                pl.semaphore_wait(
                    barrier, n_col + flag(z < n_z - 1) + flag(z > 0) + flag(skips) + flag(from_skip)
                )
        for p in range(j * SUB, (j + 1) * SUB):
            here = place[(SELF, 0, p)]
            assert here == p
            for dy in range(1, n_y):
                to = (row, col_of(lax.rem(y + n_y - dy, n_y), k))
                there = place[(FAR, dy, p)]
                first.append(copy(at_ref.at[here], at_ref.at[there], at_send.at[0],
                                  at_recv.at[there], to))
                first[-1].start()
            there = place[(SIDE, 0, p)]
            first.append(copy(at_ref.at[here], at_ref.at[there], at_send.at[0],
                              at_recv.at[there], partner))
            first[-1].start()

    kinds, dys, ps = ([c[t] for c in order] for t in range(3))

    def forward(i):
        return copy(at_ref.at[i], at_ref.at[i + 1], fw_send.at[0], at_recv.at[i + 1], partner)

    def send(src, dst, send_sem, recv_sem, i, device):
        for t in range(2):
            copy(src[t].at[i], dst[t].at[i], send_sem.at[0], recv_sem.at[i], device).start()

    def take(recv_sem, i):
        pltpu.make_async_copy(size_ref.at[i], size_ref.at[i], recv_sem.at[i]).wait()

    def fin_copy(i):
        kind, dy, p = pick(i, kinds), pick(i, dys), pick(i, ps)
        odd = lax.rem(kind, 2)
        to = (row, col_of(lax.rem(y + dy, n_y), lax.rem(k + odd, PAIR)))
        return copy(fin_ref.at[i], land_ref.at[p], f_send.at[0], f_recv.at[p], to)

    def compute(i):
        kind = pick(i, kinds)

        with jax.named_scope("wait_a"):
            @pl.when(kind != SELF)
            def _():
                copy(at_ref.at[i], at_ref.at[i], fw_send.at[0], at_recv.at[i], partner).wait_recv()

        @pl.when(kind == FAR)
        def _():
            forward(i).start()

        with jax.named_scope("dot_away"):
            lhs = at_ref[i]
            encode(jnp.dot(lhs, b_away[...], preferred_element_type=jnp.float32), xs[0].at[i], xs[1].at[i])
            send(xs, xr, x_send, x_recv, i, beside)
        with jax.named_scope("dot_own"):
            own_ref[i] = jnp.dot(lhs, b_own[...], preferred_element_type=jnp.float32)

    def combine(i):
        with jax.named_scope("wait_x"):
            take(x_recv, i)
        total_ref[...] = own_ref[i] + decode(xr[0].at[i], xr[1].at[i])

        @pl.when(from_above)
        def _():
            with jax.named_scope("wait_up"):
                take(up_recv, i)
            total_ref[...] += decode(zup[0].at[i], zup[1].at[i])

        @pl.when(from_below)
        def _():
            with jax.named_scope("wait_dn"):
                take(dn_recv, i)
            total_ref[...] += decode(zdn[0].at[i], zdn[1].at[i])

        @pl.when(jnp.logical_not(final))
        def _():
            encode(total_ref[...], zs[0].at[i], zs[1].at[i])

        @pl.when(goes_down)
        def _():
            send(zs, zup, z_send, up_recv, i, below)

        @pl.when(goes_up)
        def _():
            send(zs, zdn, z_send, dn_recv, i, above)

        @pl.when(skip_up)
        def _():
            send(zs, zdn, z_send, dn_recv, i, skip_to)

        @pl.when(skip_dn)
        def _():
            send(zs, zup, z_send, up_recv, i, skip_to)

        @pl.when(final)
        def _():
            fin_ref[i] = total_ref[...].astype(jnp.bfloat16)

            @pl.when(pick(i, kinds) != SELF)
            def _():
                fin_copy(i).start()

    inner = jnp.logical_not(final) & (from_above | from_below)
    lag = jnp.where(final, LAG_FINAL, jnp.where(inner, LAG_INNER, LAG_OUTER))

    with jax.named_scope("wait_b"):
        loads[1].wait()
        loads[2].wait()

    def main(i, carry):
        @pl.when(i < chunks)
        def _():
            compute(i)

        @pl.when((i >= lag) & (i < chunks + lag))
        def _():
            combine(i - lag)

        return carry

    lax.fori_loop(0, chunks + LAG_FINAL, main, 0)

    rows = land_ref.shape[1]

    def out(src, p):
        return pltpu.make_async_copy(src.at[p], o_ref.at[pl.ds(p * rows, rows)], out_sem.at[0])

    for p in range(pieces):
        @pl.when(final)
        def _(p=p):
            out(fin_ref, p).start()

        @pl.when(jnp.logical_not(final))
        def _(p=p):
            with jax.named_scope("wait_land"):
                copy(fin_ref.at[p], land_ref.at[p], f_send.at[0], f_recv.at[p], partner).wait_recv()
            out(land_ref, p).start()

    def drained(ref, sem):
        pltpu.make_async_copy(ref, ref, sem.at[0]).wait()

    with jax.named_scope("drain"):
        drained(at_ref.at[pl.ds(0, n_y * pieces)], at_send)
        drained(at_ref.at[pl.ds(0, (n_y - 1) * pieces)], fw_send)
        drained(size_ref, x_send)

        @pl.when(jnp.logical_not(final))
        def _():
            drained(size_ref, z_send)

        @pl.when(final)
        def _():
            drained(fin_ref.at[pl.ds(pieces, chunks - pieces)], f_send)

    with jax.named_scope("wait_out"):
        drained(o_ref, out_sem)


def per_device(n_row, n_col, tile_values, tile_counts, tile_cols, panels):
    slots, tile, _ = tile_values.shape
    deep, columns = panels.shape
    wide = columns // PAIR
    pieces = BC_DEV * SUB
    chunks = pieces * n_col
    rows = tile // SUB
    f32, bf16 = jnp.float32, jnp.bfloat16
    smem = pl.BlockSpec(memory_space=pltpu.SMEM)
    hbm = pl.BlockSpec(memory_space=pl.ANY)
    dma = pltpu.SemaphoreType.DMA
    coded = (pltpu.VMEM((chunks, rows, wide), jnp.int16), pltpu.VMEM((chunks, 1, wide), f32))
    return pl.pallas_call(
        functools.partial(kernel, n_row, n_col),
        out_shape=jax.ShapeDtypeStruct((BC_DEV * tile, wide), bf16),
        in_specs=[smem, smem, hbm, hbm],
        out_specs=hbm,
        scratch_shapes=[
            pltpu.VMEM((slots, tile, tile), bf16),
            pltpu.VMEM((deep, wide), bf16),
            pltpu.VMEM((deep, wide), bf16),
            pltpu.VMEM((chunks, rows, deep), bf16),
            pltpu.VMEM((rows, wide), f32),
            pltpu.VMEM((chunks, rows, wide), f32),
            coded,
            coded,
            coded,
            coded,
            coded,
            pltpu.VMEM((chunks, rows, wide), bf16),
            pltpu.VMEM((pieces, rows, wide), bf16),
            pltpu.VMEM((chunks, 1, (rows // 2 + 1) * wide), f32),
            dma((3,)),
            dma((1,)),
            dma((chunks,)),
            dma((1,)),
            dma((1,)),
            dma((chunks,)),
            dma((1,)),
            dma((chunks,)),
            dma((chunks,)),
            dma((1,)),
            dma((pieces,)),
            dma((1,)),
        ],
        compiler_params=pltpu.CompilerParams(
            collective_id=0, has_side_effects=True, vmem_limit_bytes=56 * 1024 * 1024
        ),
    )(tile_counts.T, tile_cols.T, tile_values, panels)


def solution(mesh):
    n_row, n_col = mesh.shape["row"], mesh.shape["col"]
    return jax.shard_map(
        functools.partial(per_device, n_row, n_col),
        mesh=mesh,
        in_specs=(P("row", "col", None), P("row", "col"), P("row", "col"), P("row", "col")),
        out_specs=P("col", "row"),
        check_vma=False,
    )
```

```python
import functools

import jax
import jax.numpy as jnp
from jax import lax
from jax.experimental import pallas as pl
from jax.experimental.pallas import tpu as pltpu
from jax.sharding import PartitionSpec as P

BC_DEV = 2
PAIR = 2
PIECES = 4
Z_WAIT = 4
LAG_OUTER = 1
LAG_INNER = 3
LAG_FINAL = 7
TOP = 32767.0
MESH = pl.DeviceIdType.MESH


class Plan:
    def __init__(self, n_y):
        self.others = n_y - 1
        self.near = 2 * BC_DEV
        self.pairs = (PIECES - 1) * self.others
        self.tails = 2 * self.others
        self.slots = self.near + self.pairs
        self.units = 2 * self.slots + self.tails
        self.hops = self.units + 1
        self.arrivals = BC_DEV + 2 * (self.pairs + self.tails)


def encode(value, code_ref, step_ref):
    peak = jnp.maximum(jnp.max(jnp.abs(value), axis=0, keepdims=True), 1e-30)
    code_ref[...] = jnp.round(value * (TOP / peak)).astype(jnp.int32).astype(jnp.int16)
    step_ref[...] = peak * (1.0 / TOP)


def decode(code_ref, step_ref):
    return code_ref[...].astype(jnp.int32).astype(jnp.float32) * step_ref[...]


def build_dense(j, counts_ref, cols_ref, tiles_ref, at_ref):
    slots, tile, _ = tiles_ref.shape
    start = jnp.int32(0)
    for i in range(counts_ref.shape[1]):
        count = counts_ref[0, i]
        here = jnp.minimum(start, slots - 1)
        after = jnp.minimum(start + 1, slots - 1)
        one = (count > 0) & (cols_ref[0, here] == j)
        two = (count > 1) & (cols_ref[0, after] == j)
        block = tiles_ref[jnp.where(two, after, here)]
        keep = jnp.where(one | two, 1.0, 0.0).astype(jnp.float32)
        at_ref[j, :, i * tile : (i + 1) * tile] = (block.astype(jnp.float32) * keep).T.astype(jnp.bfloat16)
        start = start + count


def kernel(
    n_row, n_col, counts_hbm, cols_hbm, tiles_hbm, b_hbm, o_ref,
    counts_ref, cols_ref, tiles_ref, b_away, b_own, at_ref, tail_ref, own_ref, away_ref, xs, xr, zs, zr,
    fin_ref, land_ref, size_ref, load_sem,
    a_send, a_recv, fw_send, x_send, x_recv, z_send, z_recv, f_send, f_recv, out_sem,
):
    row, col = lax.axis_index("row"), lax.axis_index("col")
    n_z, n_y = n_row // PAIR, n_col // PAIR
    plan = Plan(n_y)
    z, x = row // PAIR, lax.rem(row, PAIR)
    y, k = col // PAIR, lax.rem(col, PAIR)
    wide = b_own.shape[1]
    rows = own_ref.shape[1]
    half = rows // 2

    def row_of(z_at, x_at):
        return z_at * PAIR + x_at

    def col_of(y_at, k_at):
        return y_at * PAIR + k_at

    def load(src, dst, i):
        return pltpu.make_async_copy(src, dst, load_sem.at[i])

    at_away = pl.ds(pl.multiple_of((1 - x) * wide, wide), wide)
    at_own = pl.ds(pl.multiple_of(x * wide, wide), wide)
    loads = [
        load(tiles_hbm, tiles_ref, 0),
        load(counts_hbm, counts_ref, 3),
        load(cols_hbm, cols_ref, 4),
        load(b_hbm.at[:, at_away], b_away, 1),
        load(b_hbm.at[:, at_own], b_own, 2),
    ]
    for c in loads:
        c.start()

    beside = (row_of(z, 1 - x), col)
    partner = (row, col_of(y, 1 - k))
    final = z == col
    skip_up = (col == 0) & (z == 2)
    skip_dn = (col == n_z - 1) & (z == n_z - 3)
    low_end, high_end = (z == 0) & (col == 0), (z == n_z - 1) & (col == n_z - 1)
    skips, from_skip = skip_up | skip_dn, low_end | high_end
    from_above = (z > col) & (z < n_z - 1) & jnp.logical_not((col == 0) & (z == 1))
    from_below = (z < col) & (z > 0) & jnp.logical_not((col == n_z - 1) & (z == n_z - 2))
    inner = from_above | from_below
    outer = jnp.logical_not(final | inner)
    from_side = jnp.where(z > col, 0, 1)
    to_side = jnp.where(skips, 1 - from_side, from_side)
    z_next = jnp.where(final, jnp.where(z < n_z - 1, z + 1, z - 1), jnp.where(z > col, z - 1, z + 1))
    z_next = jnp.where(skips, jnp.minimum(col, n_z - 1), z_next)
    onward = (row_of(z_next, x), col)
    above = (row_of(jnp.minimum(z + 1, n_z - 1), x), col)
    below = (row_of(jnp.maximum(z - 1, 0), x), col)
    skip_of = (row_of(jnp.where(low_end, 2, n_z - 3), x), col)

    def flag(b):
        return jnp.where(b, 1, 0).astype(jnp.int32)

    barrier = pltpu.get_barrier_semaphore()

    def greet(device):
        pl.semaphore_signal(barrier, inc=1, device_id=device, device_id_type=MESH)

    greet(beside)
    for step in range(1, n_col):
        greet((row, lax.rem(col + step, n_col)))
    pl.when(z < n_z - 1)(lambda: greet(above))
    pl.when(z > 0)(lambda: greet(below))
    pl.when(skips)(lambda: greet(onward))
    pl.when(from_skip)(lambda: greet(skip_of))

    def copy(src, dst, send, recv, device):
        return pltpu.make_async_remote_copy(
            src_ref=src, dst_ref=dst, send_sem=send, recv_sem=recv,
            device_id=device, device_id_type=MESH,
        )

    with jax.named_scope("wait_tiles"):
        for c in loads[:3]:
            c.wait()
    for j in range(BC_DEV):
        with jax.named_scope("build"):
            build_dense(j, counts_ref, cols_ref, tiles_ref, at_ref)
        if j == 0:
            with jax.named_scope("wait_barrier"):
                pl.semaphore_wait(
                    barrier, n_col + flag(z < n_z - 1) + flag(z > 0) + flag(skips) + flag(from_skip)
                )
        for p in range(2 * j, 2 * j + 2):
            at = p % 2 * rows
            for dy in range(1, n_y):
                to = (row, col_of(lax.rem(y + n_y - dy, n_y), k))
                if p < PIECES - 1:
                    q = p * plan.others + dy - 1
                    copy(at_ref.at[j, pl.ds(at, rows)], at_ref.at[plan.near + q, pl.ds(0, rows)],
                         a_send.at[0], a_recv.at[BC_DEV + 2 * q], to).start()
                    continue
                for h in range(2):
                    t = h * plan.others + dy - 1
                    copy(at_ref.at[j, pl.ds(at + h * half, half)], tail_ref.at[t, pl.ds(0, half)],
                         a_send.at[0], a_recv.at[BC_DEV + 2 * (plan.pairs + t)], to).start()
        copy(at_ref.at[j], at_ref.at[BC_DEV + j], a_send.at[0], a_recv.at[j], partner).start()

    def send(src, dst, send_sem, recv_sem, i, device):
        for t in range(2):
            copy(src[t].at[i], dst[t], send_sem, recv_sem, device).start()

    def take(recv_sem):
        pltpu.make_async_copy(size_ref.at[0], size_ref.at[0], recv_sem).wait()

    def send_x(i, kind=0):
        send(xs, [r.at[i] for r in xr], x_send.at[kind], x_recv.at[i], i, beside)

    def send_z(u):
        send(zs, [r.at[to_side, u] for r in zr], z_send.at[0], z_recv.at[to_side, u], u, onward)

    def coded_x(i, value):
        encode(value, xs[0].at[i], xs[1].at[i])

    def coded_z(u, value):
        encode(value, zs[0].at[u], zs[1].at[u])

    def from_x(i):
        with jax.named_scope("wait_x"):
            take(x_recv.at[i])
        return decode(xr[0].at[i], xr[1].at[i])

    def from_z(side, u):
        with jax.named_scope("wait_z"):
            take(z_recv.at[side, u])
        return decode(zr[0].at[side, u], zr[1].at[side, u])

    def dot(lhs, b_ref):
        return jnp.dot(lhs, b_ref[...], preferred_element_type=jnp.float32)

    def arrival(ref, n):
        copy(ref, ref, fw_send.at[0], a_recv.at[n], partner).wait_recv()

    def forward(ref, n, size):
        first, second = ref.at[pl.ds(0, size)], ref.at[pl.ds(size, size)]
        with jax.named_scope("wait_a"):
            arrival(first, n)
        copy(first, second, fw_send.at[0], a_recv.at[n + 1], partner).start()

    def forwarded(ref, n, size):
        with jax.named_scope("wait_f"):
            arrival(ref.at[pl.ds(size, size)], n + 1)

    def compute(d):
        @pl.when((d >= BC_DEV) & (d < plan.near))
        def _():
            arrival(at_ref.at[d], d - BC_DEV)

        @pl.when(d >= plan.near)
        def _():
            forwarded(at_ref.at[d], BC_DEV + 2 * (d - plan.near), rows)

        lhs = at_ref[d]
        with jax.named_scope("dot_away"):
            away = dot(lhs, b_away)
            for t in range(2):
                coded_x(2 * d + t, away[t * rows : (t + 1) * rows])
                send_x(2 * d + t)
        with jax.named_scope("dot_own"):
            own = dot(lhs, b_own)
            for t in range(2):
                own_ref[2 * d + t] = own[t * rows : (t + 1) * rows]

    def forward_tail(t):
        forward(tail_ref.at[t], BC_DEV + 2 * (plan.pairs + t), half)

    def compute_tail(t):
        n, i = BC_DEV + 2 * (plan.pairs + t), 2 * plan.slots + t
        forwarded(tail_ref.at[t], n, half)
        lhs = tail_ref[t]
        with jax.named_scope("tail_away"):
            coded_x(i, dot(lhs, b_away))
            send_x(i)
        with jax.named_scope("tail_own"):
            own_ref[i] = dot(lhs, b_own)

        @pl.when(t + 1 < plan.tails)
        def _():
            forward_tail(t + 1)

    def work(s):
        @pl.when((lax.rem(s, 2) == 0) & (s < 2 * plan.slots))
        def _():
            compute(s // 2)

        @pl.when((lax.rem(s, 2) == 1) & (s >= 2 * plan.near - 1) & (s < 2 * plan.slots - 1))
        def _():
            d = (s + 1) // 2
            forward(at_ref.at[d], BC_DEV + 2 * (d - plan.near), rows)

        @pl.when(s == 2 * plan.slots - 1)
        def _():
            forward_tail(0)

        @pl.when((s >= 2 * plan.slots) & (s < plan.units))
        def _():
            compute_tail(s - 2 * plan.slots)

    def fin_send(i):
        def go(src, to_y, to_k, piece, at, size, sem):
            copy(src, land_ref.at[piece, pl.ds(at, size)], f_send.at[0], f_recv.at[sem],
                 (row, col_of(to_y, to_k))).start()

        @pl.when((i >= PIECES) & (i < 2 * PIECES - 1))
        def _():
            go(fin_ref.at[i], y, 1 - k, i - PIECES, 0, rows, i - PIECES)

        @pl.when(i == 2 * PIECES - 1)
        def _():
            for h in range(2):
                go(fin_ref.at[i, pl.ds(h * half, half)], y, 1 - k, PIECES - 1, h * half, half, PIECES - 1 + h)

        @pl.when((i >= 2 * PIECES) & (i < 2 * plan.slots))
        def _():
            q = i // 2 - plan.near
            p, dy = q // plan.others, lax.rem(q, plan.others) + 1
            go(fin_ref.at[i], lax.rem(y + dy, n_y), lax.rem(k + lax.rem(i, 2), PAIR), p, 0, rows, p)

        @pl.when(i >= 2 * plan.slots)
        def _():
            t = i - 2 * plan.slots
            h, dy = t // plan.others, lax.rem(t, plan.others) + 1
            for odd in range(2):
                go(fin_ref.at[i, pl.ds(odd * half, half)], lax.rem(y + dy, n_y), lax.rem(k + odd, PAIR),
                   PIECES - 1, h * half, half, PIECES - 1 + h)

    with jax.named_scope("wait_b"):
        loads[3].wait()
    with jax.named_scope("dot_first"):
        away = dot(at_ref[0], b_away)
        coded_x(0, away[:rows])
        send_x(0)
        away_ref[...] = away[rows:]

        @pl.when(outer)
        def _():
            coded_z(0, away_ref[...])
            send_z(0)

    loads[4].wait()
    with jax.named_scope("dot_first_own"):
        own = dot(at_ref[0], b_own)
        own_ref[0] = own[:rows]
        own_ref[1] = own[rows:]

        @pl.when(outer)
        def _():
            coded_z(1, own_ref[1])
            send_z(1)

    def loop(lag, early, combine):
        def body(s, carry):
            work(s)
            e = s - lag
            if early is not None:
                pl.when(e == 0)(lambda: early(0))
                pl.when(e == 1)(lambda: early(1))

            @pl.when((e >= 2) & (e < plan.hops))
            def _():
                combine(e, jnp.where(e == 2, 0, e - 1))

            return carry

        lax.fori_loop(2, plan.hops + lag, body, 0)

    @pl.when(outer)
    def _():
        def combine(u, i):
            coded_z(u, own_ref[i] + from_x(i))
            send_z(u)

        loop(LAG_OUTER, None, combine)

    @pl.when(inner)
    def _():
        def early(u):
            coded_z(u, (own_ref[1] if u else away_ref[...]) + from_z(from_side, u))
            send_z(u)

        def combine(u, i):
            coded_z(u, own_ref[i] + from_x(i) + from_z(from_side, u))
            send_z(u)

        loop(LAG_INNER, early, combine)

    @pl.when(final)
    def _():
        def early(u):
            total = (own_ref[1] if u else away_ref[...]) + from_z(0, u) + from_z(1, u)
            if u:
                own_ref[1] = total
            else:
                coded_x(1, total)
                send_x(1, 1)

        def combine(u, i):
            total = own_ref[i] + from_x(i) + from_z(0, u) + from_z(1, u)
            fin_ref[i] = total.astype(jnp.bfloat16)
            fin_send(i)

            @pl.when(u == 2 + Z_WAIT)
            def _():
                fin_ref[1] = (own_ref[1] + from_x(1)).astype(jnp.bfloat16)

        loop(LAG_FINAL, early, combine)

    def out(src, p, at, size):
        here = pl.ds(at, size)
        return pltpu.make_async_copy(src.at[p, here], o_ref.at[p, here], out_sem.at[0])

    for p, at, size, sem in [(p, 0, rows, p) for p in range(PIECES - 1)] + [
        (PIECES - 1, h * half, half, PIECES - 1 + h) for h in range(2)
    ]:
        @pl.when(final)
        def _(p=p, at=at, size=size):
            out(fin_ref, p, at, size).start()

        @pl.when(jnp.logical_not(final))
        def _(p=p, at=at, size=size, sem=sem):
            here = land_ref.at[p, pl.ds(at, size)]
            with jax.named_scope("wait_land"):
                copy(here, here, f_send.at[0], f_recv.at[sem], partner).wait_recv()
            out(land_ref, p, at, size).start()

    def drained(ref, sem, t=0):
        pltpu.make_async_copy(ref, ref, sem.at[t]).wait()

    with jax.named_scope("drain"):
        drained(at_ref.at[pl.ds(0, n_y * BC_DEV)], a_send)
        drained(at_ref.at[pl.ds(0, plan.others * BC_DEV)], fw_send)
        drained(size_ref.at[pl.ds(0, plan.units - 1)], x_send)

        @pl.when(jnp.logical_not(final))
        def _():
            drained(size_ref, z_send)

        @pl.when(final)
        def _():
            drained(size_ref.at[0], x_send, 1)
            drained(fin_ref.at[pl.ds(PIECES, plan.units - PIECES)], f_send)

    with jax.named_scope("wait_out"):
        drained(o_ref, out_sem)


def per_device(n_row, n_col, tile_values, tile_counts, tile_cols, panels):
    slots, tile, _ = tile_values.shape
    deep, columns = panels.shape
    wide = columns // PAIR
    plan = Plan(n_col // PAIR)
    rows = BC_DEV * tile // PIECES
    f32, bf16, i16 = jnp.float32, jnp.bfloat16, jnp.int16
    hbm = pl.BlockSpec(memory_space=pl.ANY)
    dma = pltpu.SemaphoreType.DMA

    def coded(*lead):
        return pltpu.VMEM((*lead, rows, wide), i16), pltpu.VMEM((*lead, 1, wide), f32)

    out = pl.pallas_call(
        functools.partial(kernel, n_row, n_col),
        out_shape=pltpu.VMEM((PIECES, rows, wide), bf16),
        in_specs=[hbm] * 4,
        out_specs=pl.BlockSpec(memory_space=pltpu.VMEM),
        scratch_shapes=[
            pltpu.SMEM(tile_counts.shape[::-1], jnp.int32),
            pltpu.SMEM(tile_cols.shape[::-1], jnp.int32),
            pltpu.VMEM((slots, tile, tile), bf16),
            pltpu.VMEM((deep, wide), bf16),
            pltpu.VMEM((deep, wide), bf16),
            pltpu.VMEM((plan.slots, 2 * rows, deep), bf16),
            pltpu.VMEM((plan.tails, rows, deep), bf16),
            pltpu.VMEM((plan.units, rows, wide), f32),
            pltpu.VMEM((rows, wide), f32),
            coded(plan.units),
            coded(plan.units),
            coded(plan.hops),
            coded(2, plan.hops),
            pltpu.VMEM((plan.units, rows, wide), bf16),
            pltpu.VMEM((PIECES, rows, wide), bf16),
            pltpu.VMEM((plan.hops, 1, (rows // 2 + 1) * wide), f32),
            dma((5,)),
            dma((1,)),
            dma((plan.arrivals,)),
            dma((1,)),
            dma((2,)),
            dma((plan.units,)),
            dma((1,)),
            dma((2, plan.hops)),
            dma((1,)),
            dma((PIECES + 1,)),
            dma((1,)),
        ],
        compiler_params=pltpu.CompilerParams(
            collective_id=0, has_side_effects=True, vmem_limit_bytes=56 * 1024 * 1024
        ),
    )(tile_counts.T, tile_cols.T, tile_values, panels)
    return out.reshape(BC_DEV * tile, wide)


def solution(mesh):
    n_row, n_col = mesh.shape["row"], mesh.shape["col"]
    return jax.shard_map(
        functools.partial(per_device, n_row, n_col),
        mesh=mesh,
        in_specs=(P("row", "col", None), P("row", "col"), P("row", "col"), P("row", "col")),
        out_specs=P("col", "row"),
        check_vma=False,
    )
```

```python
import functools

import jax
import jax.numpy as jnp
from jax import lax
from jax.experimental import pallas as pl
from jax.experimental.pallas import tpu as pltpu
from jax.sharding import PartitionSpec as P

BC_DEV = 2
PAIR = 2
PIECES = 4
CUTS = 2
Z_WAIT = 4
LATE = 2
LAG_OUTER = 1
LAG_INNER = 3
LAG_FINAL = 7
TOP = 32767.0
MESH = pl.DeviceIdType.MESH


class Plan:
    def __init__(self, n_y):
        self.others = n_y - 1
        self.near = 2 * BC_DEV
        self.pairs = (PIECES - 1) * self.others
        self.tails = CUTS * self.others
        self.slots = self.near + self.pairs
        self.units = 2 * self.slots + self.tails
        self.hops = self.units + 1
        self.large = self.hops - self.tails
        self.arrivals = BC_DEV + 2 * (self.pairs + self.tails)


def encode(value, code_ref, step_ref):
    peak = jnp.maximum(jnp.max(jnp.abs(value), axis=0, keepdims=True), 1e-30)
    code_ref[...] = jnp.round(value * (TOP / peak)).astype(jnp.int32).astype(jnp.int16)
    step_ref[...] = peak * (1.0 / TOP)


def decode(code_ref, step_ref):
    return code_ref[...].astype(jnp.int32).astype(jnp.float32) * step_ref[...]


def build_dense(j, counts_ref, cols_ref, tiles_ref, at_ref):
    slots, tile, _ = tiles_ref.shape
    start = jnp.int32(0)
    for i in range(counts_ref.shape[1]):
        count = counts_ref[0, i]
        here = jnp.minimum(start, slots - 1)
        after = jnp.minimum(start + 1, slots - 1)
        one = (count > 0) & (cols_ref[0, here] == j)
        two = (count > 1) & (cols_ref[0, after] == j)
        block = tiles_ref[jnp.where(two, after, here)]
        keep = jnp.where(one | two, 1.0, 0.0).astype(jnp.float32)
        at_ref[j, :, i * tile : (i + 1) * tile] = (block.astype(jnp.float32) * keep).T.astype(jnp.bfloat16)
        start = start + count


def kernel(
    n_row, n_col, counts_hbm, cols_hbm, tiles_hbm, b_hbm, o_ref,
    counts_ref, cols_ref, tiles_ref, b_away, b_own, at_ref, tail_ref, own_ref, away_ref, xs, xr, zs, zr, oi,
    fin_ref, land_ref, size_ref, small_ref, x_size_ref, z_size_ref, large_size_ref,
    cut_ref, o_size_ref, load_sem,
    a_send, a_recv, fw_send, x_send, x_recv, z_send, z_recv, o_send, o_recv, f_send, f_recv, out_sem,
):
    row, col = lax.axis_index("row"), lax.axis_index("col")
    n_z, n_y = n_row // PAIR, n_col // PAIR
    plan = Plan(n_y)
    z, x = row // PAIR, lax.rem(row, PAIR)
    y, k = col // PAIR, lax.rem(col, PAIR)
    wide = b_own.shape[1]
    rows = own_ref.shape[1]
    cut = rows // CUTS
    small = 2 * cut

    def row_of(z_at, x_at):
        return z_at * PAIR + x_at

    def col_of(y_at, k_at):
        return y_at * PAIR + k_at

    def load(src, dst, i):
        return pltpu.make_async_copy(src, dst, load_sem.at[i])

    at_away = pl.ds(pl.multiple_of((1 - x) * wide, wide), wide)
    at_own = pl.ds(pl.multiple_of(x * wide, wide), wide)
    loads = [
        load(tiles_hbm, tiles_ref, 0),
        load(counts_hbm, counts_ref, 3),
        load(cols_hbm, cols_ref, 4),
        load(b_hbm.at[:, at_away], b_away, 1),
        load(b_hbm.at[:, at_own], b_own, 2),
    ]
    for c in loads:
        c.start()

    beside = (row_of(z, 1 - x), col)
    partner = (row, col_of(y, 1 - k))
    final = z == col
    skip_up = (col == 0) & (z == 2)
    skip_dn = (col == n_z - 1) & (z == n_z - 3)
    low_end, high_end = (z == 0) & (col == 0), (z == n_z - 1) & (col == n_z - 1)
    skips, from_skip = skip_up | skip_dn, low_end | high_end
    from_above = (z > col) & (z < n_z - 1) & jnp.logical_not((col == 0) & (z == 1))
    from_below = (z < col) & (z > 0) & jnp.logical_not((col == n_z - 1) & (z == n_z - 2))
    inner = from_above | from_below
    outer = jnp.logical_not(final | inner)
    from_side = jnp.where(z > col, 0, 1)
    to_side = jnp.where(skips, 1 - from_side, from_side)
    z_next = jnp.where(final, jnp.where(z < n_z - 1, z + 1, z - 1), jnp.where(z > col, z - 1, z + 1))
    z_next = jnp.where(skips, jnp.minimum(col, n_z - 1), z_next)
    onward = (row_of(z_next, x), col)
    above = (row_of(jnp.minimum(z + 1, n_z - 1), x), col)
    below = (row_of(jnp.maximum(z - 1, 0), x), col)
    skip_of = (row_of(jnp.where(low_end, 2, n_z - 3), x), col)

    owners = n_z == 4 and n_y == 2
    owner = owners & (z // 2 != y)
    owner_row = row_of(jnp.minimum(col, n_z - 1), x)
    bringer = (row_of(jnp.where(z < 2, 2, 1), x), jnp.minimum(z, n_col - 1))

    def flag(b):
        return jnp.where(b, 1, 0).astype(jnp.int32)

    barrier = pltpu.get_barrier_semaphore()

    def greet(device):
        pl.semaphore_signal(barrier, inc=1, device_id=device, device_id_type=MESH)

    greet(beside)
    for step in range(1, n_col):
        greet((row, lax.rem(col + step, n_col)))
    pl.when(z < n_z - 1)(lambda: greet(above))
    pl.when(z > 0)(lambda: greet(below))
    pl.when(skips)(lambda: greet(onward))
    pl.when(from_skip)(lambda: greet(skip_of))
    if owners:
        pl.when(owner)(lambda: greet(bringer))
        for k_at in range(PAIR):
            pl.when(inner)(lambda k_at=k_at: greet((owner_row, col_of(1 - y, k_at))))

    def copy(src, dst, send, recv, device):
        return pltpu.make_async_remote_copy(
            src_ref=src, dst_ref=dst, send_sem=send, recv_sem=recv,
            device_id=device, device_id_type=MESH,
        )

    with jax.named_scope("wait_tiles"):
        for c in loads[:3]:
            c.wait()
    for j in range(BC_DEV):
        with jax.named_scope("build"):
            build_dense(j, counts_ref, cols_ref, tiles_ref, at_ref)
        if j == 0:
            with jax.named_scope("wait_barrier"):
                pl.semaphore_wait(
                    barrier, n_col + flag(z < n_z - 1) + flag(z > 0) + flag(skips) + flag(from_skip)
                    + (flag(owner) + PAIR * flag(inner) if owners else 0)
                )
        for p in range(2 * j, 2 * j + 2):
            at = p % 2 * rows
            for dy in range(1, n_y):
                to = (row, col_of(lax.rem(y + n_y - dy, n_y), k))
                if p < PIECES - 1:
                    q = p * plan.others + dy - 1
                    copy(at_ref.at[j, pl.ds(at, rows)], at_ref.at[plan.near + q, pl.ds(0, rows)],
                         a_send.at[0], a_recv.at[BC_DEV + 2 * q], to).start()
                    continue
                for h in range(CUTS):
                    t = h * plan.others + dy - 1
                    copy(at_ref.at[j, pl.ds(at + h * cut, cut)], tail_ref.at[t, pl.ds(0, cut)],
                         a_send.at[0], a_recv.at[BC_DEV + 2 * (plan.pairs + t)], to).start()
        copy(at_ref.at[j], at_ref.at[BC_DEV + j], a_send.at[0], a_recv.at[j], partner).start()

    def first(ref, at, size):
        return ref.at[at] if size == rows else ref.at[(*at, pl.ds(0, size))]

    def send(src, i, dst, at, size, send_sem, recv_sem, device):
        copy(first(src[0], (i,), size), first(dst[0], at, size), send_sem, recv_sem, device).start()
        copy(src[1].at[i], dst[1].at[at], send_sem, recv_sem, device).start()

    def taken(ref, at, size, recv_sem):
        both = size_ref if size == rows else small_ref
        pltpu.make_async_copy(both, both, recv_sem).wait()
        return decode(first(ref[0], at, size), ref[1].at[at])

    def send_x(i, value, kind=0):
        size = value.shape[0]
        encode(value, first(xs[0], (i,), size), xs[1].at[i])
        send(xs, i, xr, (i,), size, x_send.at[kind], x_recv.at[i], beside)

    def code_z(u, value):
        encode(value, first(zs[0], (u,), value.shape[0]), zs[1].at[u])

    def send_z(u, value):
        code_z(u, value)
        send(zs, u, zr, (to_side, u), value.shape[0], z_send.at[0], z_recv.at[to_side, u], onward)

    def send_owners(u, value, which):
        code_z(u, value)
        t = u - plan.large
        for odd in range(PAIR):
            to = (owner_row, col_of(1 - y, lax.rem(k + odd, PAIR)))
            for src, dst in ((zs[0].at[u, pl.ds(odd * cut, cut)], oi[0]), (zs[1].at[u], oi[1])):
                copy(src, dst.at[which, t], o_send.at[0], o_recv.at[which, t], to).start()

    def from_owner(which, t):
        with jax.named_scope("wait_o"):
            pltpu.make_async_copy(cut_ref, cut_ref, o_recv.at[which, t]).wait()
        return decode(oi[0].at[which, t], oi[1].at[which, t])

    def from_x(i, size):
        with jax.named_scope("wait_x"):
            return taken(xr, (i,), size, x_recv.at[i])

    def from_z(side, u, size):
        with jax.named_scope("wait_z"):
            return taken(zr, (side, u), size, z_recv.at[side, u])

    def dot(lhs, b_ref):
        return jnp.dot(lhs, b_ref[...], preferred_element_type=jnp.float32)

    def arrival(ref, n):
        copy(ref, ref, fw_send.at[0], a_recv.at[n], partner).wait_recv()

    def forward(ref, n, size):
        first, second = ref.at[pl.ds(0, size)], ref.at[pl.ds(size, size)]
        with jax.named_scope("wait_a"):
            arrival(first, n)
        copy(first, second, fw_send.at[0], a_recv.at[n + 1], partner).start()

    def forwarded(ref, n, size):
        with jax.named_scope("wait_f"):
            arrival(ref.at[pl.ds(size, size)], n + 1)

    def compute(d):
        @pl.when((d >= BC_DEV) & (d < plan.near))
        def _():
            arrival(at_ref.at[d], d - BC_DEV)

        @pl.when(d >= plan.near)
        def _():
            forwarded(at_ref.at[d], BC_DEV + 2 * (d - plan.near), rows)

        lhs = at_ref[d]
        with jax.named_scope("dot_away"):
            away = dot(lhs, b_away)
            for t in range(2):
                send_x(2 * d + t, away[t * rows : (t + 1) * rows])
        with jax.named_scope("dot_own"):
            own = dot(lhs, b_own)
            for t in range(2):
                own_ref[2 * d + t] = own[t * rows : (t + 1) * rows]

    def forward_tail(t):
        forward(tail_ref.at[t], BC_DEV + 2 * (plan.pairs + t), cut)

    def tail_away(t):
        n, i = BC_DEV + 2 * (plan.pairs + t), 2 * plan.slots + t

        @pl.when(t + 1 < plan.tails)
        def _():
            forward_tail(t + 1)

        forwarded(tail_ref.at[t], n, cut)
        with jax.named_scope("tail_away"):
            send_x(i, dot(tail_ref[t], b_away))

    def tail_own(g):
        both = tail_ref[pl.ds(2 * g, 2)].reshape(2 * small, tail_ref.shape[2])
        with jax.named_scope("tail_own"):
            own = dot(both, b_own)
            for t in range(2):
                own_ref[2 * plan.slots + 2 * g + t, pl.ds(0, small)] = own[t * small : (t + 1) * small]

    def work(s):
        @pl.when((lax.rem(s, 2) == 0) & (s < 2 * plan.slots))
        def _():
            compute(s // 2)

        @pl.when((lax.rem(s, 2) == 1) & (s >= 2 * plan.near - 1) & (s < 2 * plan.slots - 1))
        def _():
            d = (s + 1) // 2
            forward(at_ref.at[d], BC_DEV + 2 * (d - plan.near), rows)

        m = s - (2 * plan.slots - 1)

        @pl.when(m == 0)
        def _():
            forward_tail(0)
            tail_away(0)

        @pl.when((m >= 1) & (2 * m <= plan.tails))
        def _():
            tail_away(2 * m - 1)
            tail_own(m - 1)

        @pl.when((m >= 1) & (2 * m < plan.tails))
        def _():
            tail_away(2 * m)

    def fin_send(i, tail):
        def go(src, to_y, to_k, piece, at, size, sem):
            copy(src, land_ref.at[piece, pl.ds(at, size)], f_send.at[0], f_recv.at[sem],
                 (row, col_of(to_y, to_k))).start()

        def cuts(h, src, at, to_y, to_k):
            go(src.at[i, pl.ds(at, cut)], to_y, to_k, PIECES - 1, h * cut, cut, PIECES - 1 + h)

        if tail:
            t = i - 2 * plan.slots
            h, dy = t // plan.others, lax.rem(t, plan.others) + 1
            for odd in range(2):
                cuts(h, fin_ref, odd * cut, lax.rem(y + dy, n_y), lax.rem(k + odd, PAIR))
            return

        @pl.when((i >= PIECES) & (i < 2 * PIECES - 1))
        def _():
            go(fin_ref.at[i], y, 1 - k, i - PIECES, 0, rows, i - PIECES)

        @pl.when(i == 2 * PIECES - 1)
        def _():
            for h in range(CUTS):
                cuts(h, fin_ref, h * cut, y, 1 - k)

        @pl.when(i >= 2 * PIECES)
        def _():
            q = i // 2 - plan.near
            p, dy = q // plan.others, lax.rem(q, plan.others) + 1
            go(fin_ref.at[i], lax.rem(y + dy, n_y), lax.rem(k + lax.rem(i, 2), PAIR), p, 0, rows, p)

    with jax.named_scope("wait_b"):
        loads[3].wait()
    with jax.named_scope("dot_first"):
        away = dot(at_ref[0], b_away)
        send_x(0, away[:rows])
        away_ref[...] = away[rows:]

        @pl.when(outer)
        def _():
            send_z(0, away_ref[...])

    loads[4].wait()
    with jax.named_scope("dot_first_own"):
        own = dot(at_ref[0], b_own)
        own_ref[0] = own[:rows]
        own_ref[1] = own[rows:]

        @pl.when(outer)
        def _():
            send_z(1, own_ref[1])

    def loop(lag, early, combine, late=0):
        def body(s, carry):
            work(s)
            e = s - lag
            if early is not None:
                pl.when(e == 0)(lambda: early(0))
                pl.when(e == 1)(lambda: early(1))

            tails_at = plan.large - late
            tail = (e >= tails_at) & (e < tails_at + plan.tails)

            @pl.when((e >= 2) & (e < plan.hops) & jnp.logical_not(tail))
            def _():
                u = jnp.where(e < tails_at, e, e - plan.tails)
                combine(u, jnp.where(u == 2, 0, u - 1), rows, False)

            @pl.when(tail)
            def _():
                combine(e + late, e + late - 1, small, True)

            return carry

        lax.fori_loop(2, plan.hops + lag, body, 0)

    def own(i, size):
        return first(own_ref, (i,), size)[...]

    @pl.when(outer)
    def _():
        def combine(u, i, size, tail):
            send_z(u, own(i, size) + from_x(i, size))

        loop(LAG_OUTER, None, combine)

    @pl.when(inner)
    def _():
        def early(u):
            send_z(u, (own_ref[1] if u else away_ref[...]) + from_z(from_side, u, rows))

        def combine(u, i, size, tail):
            total = own(i, size) + from_x(i, size) + from_z(from_side, u, size)
            if tail and owners:
                send_owners(u, total, 0)
            else:
                send_z(u, total)

        loop(LAG_INNER, early, combine)

    @pl.when(final)
    def _():
        def early(u):
            total = (own_ref[1] if u else away_ref[...]) + from_z(0, u, rows) + from_z(1, u, rows)
            if u:
                own_ref[1] = total
            else:
                send_x(1, total, 1)

        def combine(u, i, size, tail):
            total = own(i, size) + from_x(i, size)
            if tail and owners:
                send_owners(u, total + from_z(k, u, size), 1)
                return
            total += from_z(0, u, size) + from_z(1, u, size)
            first(fin_ref, (i,), size)[...] = total.astype(jnp.bfloat16)
            fin_send(i, tail)

            if not tail:
                @pl.when(u == 2 + Z_WAIT)
                def _():
                    fin_ref[1] = (own_ref[1] + from_x(1, rows)).astype(jnp.bfloat16)

        loop(LAG_FINAL, early, combine, LATE if owners else 0)

    def out(src, p, at, size):
        here = pl.ds(at, size)
        return pltpu.make_async_copy(src.at[p, here], o_ref.at[p, here], out_sem.at[0])

    def hand_over(p, at, size, sem):
        @pl.when(final)
        def _():
            out(fin_ref, p, at, size).start()

        @pl.when(jnp.logical_not(final))
        def _():
            here = land_ref.at[p, pl.ds(at, size)]
            with jax.named_scope("wait_land"):
                copy(here, here, f_send.at[0], f_recv.at[sem], partner).wait_recv()
            out(land_ref, p, at, size).start()

    def hand_over_cuts():
        for h in range(CUTS):
            hand_over(PIECES - 1, h * cut, cut, PIECES - 1 + h)

    for p in range(PIECES - 1):
        hand_over(p, 0, rows, p)
    if owners:
        pl.when(jnp.logical_not(owner))(hand_over_cuts)

        @pl.when(owner)
        def _():
            for t in range(CUTS):
                o_ref[PIECES - 1, pl.ds(t * cut, cut)] = (from_owner(1, t) + from_owner(0, t)).astype(jnp.bfloat16)
    else:
        hand_over_cuts()

    def drained(ref, sem, t=0):
        pltpu.make_async_copy(ref, ref, sem.at[t]).wait()

    with jax.named_scope("drain"):
        drained(at_ref.at[pl.ds(0, n_y * BC_DEV)], a_send)
        drained(at_ref.at[pl.ds(0, plan.others * BC_DEV)], fw_send)
        drained(x_size_ref, x_send)

        if owners:
            pl.when(outer)(lambda: drained(z_size_ref, z_send))
            pl.when(inner)(lambda: drained(large_size_ref, z_send))
            pl.when(jnp.logical_not(outer))(lambda: drained(o_size_ref, o_send))
        else:
            pl.when(jnp.logical_not(final))(lambda: drained(z_size_ref, z_send))

        @pl.when(final)
        def _():
            drained(size_ref, x_send, 1)
            sent = 2 * plan.slots if owners else PIECES * n_col
            drained(fin_ref.at[pl.ds(PIECES, sent - PIECES)], f_send)

    with jax.named_scope("wait_out"):
        if owners:
            pl.when(owner)(lambda: drained(o_ref.at[pl.ds(0, PIECES - 1)], out_sem))
            pl.when(jnp.logical_not(owner))(lambda: drained(o_ref, out_sem))
        else:
            drained(o_ref, out_sem)


def per_device(n_row, n_col, tile_values, tile_counts, tile_cols, panels):
    slots, tile, _ = tile_values.shape
    deep, columns = panels.shape
    wide = columns // PAIR
    plan = Plan(n_col // PAIR)
    rows = BC_DEV * tile // PIECES
    cut = rows // CUTS
    f32, bf16, i16 = jnp.float32, jnp.bfloat16, jnp.int16
    hbm = pl.BlockSpec(memory_space=pl.ANY)
    dma = pltpu.SemaphoreType.DMA

    def coded(*lead):
        return pltpu.VMEM((*lead, rows, wide), i16), pltpu.VMEM((*lead, 1, wide), f32)

    def words(large, small):
        return pltpu.VMEM((1, (large * (rows // 2 + 1) + small * (rows // CUTS + 1)) * wide), f32)

    out = pl.pallas_call(
        functools.partial(kernel, n_row, n_col),
        out_shape=pltpu.VMEM((PIECES, rows, wide), bf16),
        in_specs=[hbm] * 4,
        out_specs=pl.BlockSpec(memory_space=pltpu.VMEM),
        scratch_shapes=[
            pltpu.SMEM(tile_counts.shape[::-1], jnp.int32),
            pltpu.SMEM(tile_cols.shape[::-1], jnp.int32),
            pltpu.VMEM((slots, tile, tile), bf16),
            pltpu.VMEM((deep, wide), bf16),
            pltpu.VMEM((deep, wide), bf16),
            pltpu.VMEM((plan.slots, 2 * rows, deep), bf16),
            pltpu.VMEM((plan.tails, 2 * rows // CUTS, deep), bf16),
            pltpu.VMEM((plan.units, rows, wide), f32),
            pltpu.VMEM((rows, wide), f32),
            coded(plan.units),
            coded(plan.units),
            coded(plan.hops),
            coded(2, plan.hops),
            (pltpu.VMEM((2, CUTS, cut, wide), i16), pltpu.VMEM((2, CUTS, 1, wide), f32)),
            pltpu.VMEM((plan.units, rows, wide), bf16),
            pltpu.VMEM((PIECES, rows, wide), bf16),
            words(1, 0),
            words(0, 1),
            words(plan.large - 2, plan.tails),
            words(plan.large, plan.tails),
            words(plan.large, 0),
            pltpu.VMEM((1, (cut // 2 + 1) * wide), f32),
            pltpu.VMEM((1, PAIR * CUTS * (cut // 2 + 1) * wide), f32),
            dma((5,)),
            dma((1,)),
            dma((plan.arrivals,)),
            dma((1,)),
            dma((2,)),
            dma((plan.units,)),
            dma((1,)),
            dma((2, plan.hops)),
            dma((1,)),
            dma((2, CUTS)),
            dma((1,)),
            dma((PIECES - 1 + CUTS,)),
            dma((1,)),
        ],
        compiler_params=pltpu.CompilerParams(
            collective_id=0, has_side_effects=True, vmem_limit_bytes=56 * 1024 * 1024
        ),
    )(tile_counts.T, tile_cols.T, tile_values, panels)
    return out.reshape(BC_DEV * tile, wide)


def solution(mesh):
    n_row, n_col = mesh.shape["row"], mesh.shape["col"]
    return jax.shard_map(
        functools.partial(per_device, n_row, n_col),
        mesh=mesh,
        in_specs=(P("row", "col", None), P("row", "col"), P("row", "col"), P("row", "col")),
        out_specs=P("col", "row"),
        check_vma=False,
    )
```

```python
import functools

import jax
import jax.numpy as jnp
from jax import lax
from jax.experimental import pallas as pl
from jax.experimental.pallas import tpu as pltpu
from jax.sharding import PartitionSpec as P

BC_DEV = 2
PAIR = 2
PIECES = 4
CUTS = 2
Z_WAIT = 4
LATE = 5
LAG_OUTER = 1
LAG_INNER = 3
LAG_FINAL = 7
TOP = 32767.0
MESH = pl.DeviceIdType.MESH


class Plan:
    def __init__(self, n_y):
        self.others = n_y - 1
        self.near = 2 * BC_DEV
        self.pairs = (PIECES - 1) * self.others
        self.tails = CUTS * self.others
        self.slots = self.near + self.pairs
        self.units = 2 * self.slots + self.tails
        self.hops = self.units + 1
        self.large = self.hops - self.tails
        self.arrivals = BC_DEV + 2 * (self.pairs + self.tails)


def encode(value, code_ref, step_ref):
    peak = jnp.maximum(jnp.max(jnp.abs(value), axis=0, keepdims=True), 1e-30)
    code_ref[...] = jnp.round(value * (TOP / peak)).astype(jnp.int32).astype(jnp.int16)
    step_ref[...] = peak * (1.0 / TOP)


def decode(code_ref, step_ref):
    return code_ref[...].astype(jnp.int32).astype(jnp.float32) * step_ref[...]


def build_dense(j, counts_ref, cols_ref, tiles_ref, at_ref):
    slots, tile, _ = tiles_ref.shape
    start = jnp.int32(0)
    for i in range(counts_ref.shape[1]):
        count = counts_ref[0, i]
        here = jnp.minimum(start, slots - 1)
        after = jnp.minimum(start + 1, slots - 1)
        one = (count > 0) & (cols_ref[0, here] == j)
        two = (count > 1) & (cols_ref[0, after] == j)
        block = tiles_ref[jnp.where(two, after, here)]
        keep = jnp.where(one | two, 1.0, 0.0).astype(jnp.float32)
        at_ref[j, :, i * tile : (i + 1) * tile] = (block.astype(jnp.float32) * keep).T.astype(jnp.bfloat16)
        start = start + count


def kernel(
    n_row, n_col, counts_hbm, cols_hbm, tiles_hbm, b_hbm, o_ref,
    counts_ref, cols_ref, tiles_ref, b_away, b_own, at_ref, tail_ref, own_ref, away_ref, xs, xr, zs, zr, part,
    fin_ref, land_ref, size_ref, small_ref, x_size_ref, z_size_ref, large_size_ref,
    parts_size_ref, load_sem,
    a_send, a_recv, fw_send, x_send, x_recv, z_send, z_recv, p_recv, f_send, f_recv, out_sem,
):
    row, col = lax.axis_index("row"), lax.axis_index("col")
    n_z, n_y = n_row // PAIR, n_col // PAIR
    plan = Plan(n_y)
    z, x = row // PAIR, lax.rem(row, PAIR)
    y, k = col // PAIR, lax.rem(col, PAIR)
    wide = b_own.shape[1]
    rows = own_ref.shape[1]
    cut = rows // CUTS
    small = 2 * cut

    def row_of(z_at, x_at):
        return z_at * PAIR + x_at

    def col_of(y_at, k_at):
        return y_at * PAIR + k_at

    def load(src, dst, i):
        return pltpu.make_async_copy(src, dst, load_sem.at[i])

    at_away = pl.ds(pl.multiple_of((1 - x) * wide, wide), wide)
    at_own = pl.ds(pl.multiple_of(x * wide, wide), wide)
    loads = [
        load(tiles_hbm, tiles_ref, 0),
        load(counts_hbm, counts_ref, 3),
        load(cols_hbm, cols_ref, 4),
        load(b_hbm.at[:, at_away], b_away, 1),
        load(b_hbm.at[:, at_own], b_own, 2),
    ]
    for c in loads:
        c.start()

    beside = (row_of(z, 1 - x), col)
    partner = (row, col_of(y, 1 - k))
    final = z == col
    skip_up = (col == 0) & (z == 2)
    skip_dn = (col == n_z - 1) & (z == n_z - 3)
    low_end, high_end = (z == 0) & (col == 0), (z == n_z - 1) & (col == n_z - 1)
    skips, from_skip = skip_up | skip_dn, low_end | high_end
    from_above = (z > col) & (z < n_z - 1) & jnp.logical_not((col == 0) & (z == 1))
    from_below = (z < col) & (z > 0) & jnp.logical_not((col == n_z - 1) & (z == n_z - 2))
    inner = from_above | from_below
    outer = jnp.logical_not(final | inner)
    from_side = jnp.where(z > col, 0, 1)
    to_side = jnp.where(skips, 1 - from_side, from_side)
    z_next = jnp.where(final, jnp.where(z < n_z - 1, z + 1, z - 1), jnp.where(z > col, z - 1, z + 1))
    z_next = jnp.where(skips, jnp.minimum(col, n_z - 1), z_next)
    onward = (row_of(z_next, x), col)
    above = (row_of(jnp.minimum(z + 1, n_z - 1), x), col)
    below = (row_of(jnp.maximum(z - 1, 0), x), col)
    skip_of = (row_of(jnp.where(low_end, 2, n_z - 3), x), col)

    owners = n_z == 4 and n_y == 2
    owner = owners & (z // 2 != y)
    near = outer & (z // 2 == y)
    owner_row = row_of(jnp.minimum(col, n_z - 1), x)
    bringer = (row_of(jnp.where(z < 2, 2, 1), x), jnp.minimum(z, n_col - 1))
    inner_of = (row_of(jnp.where(y == 0, 2, 1), x), col)
    apart = (col == 1) & ((z == 0) | (z == 2)) | (col == 2) & ((z == 3) | (z == 1))
    apart_from = (row_of(jnp.clip(2 * col - z, 0, n_z - 1), x), col)

    def flag(b):
        return jnp.where(b, 1, 0).astype(jnp.int32)

    barrier = pltpu.get_barrier_semaphore()

    def greet(device):
        pl.semaphore_signal(barrier, inc=1, device_id=device, device_id_type=MESH)

    greet(beside)
    for step in range(1, n_col):
        greet((row, lax.rem(col + step, n_col)))
    pl.when(z < n_z - 1)(lambda: greet(above))
    pl.when(z > 0)(lambda: greet(below))
    pl.when(skips)(lambda: greet(onward))
    pl.when(from_skip)(lambda: greet(skip_of))
    if owners:
        pl.when(owner)(lambda: greet(bringer))
        pl.when(apart)(lambda: greet(apart_from))
        for k_at in range(PAIR):
            pl.when(inner)(lambda k_at=k_at: greet((owner_row, col_of(1 - y, k_at))))

    def copy(src, dst, send, recv, device):
        return pltpu.make_async_remote_copy(
            src_ref=src, dst_ref=dst, send_sem=send, recv_sem=recv,
            device_id=device, device_id_type=MESH,
        )

    with jax.named_scope("wait_tiles"):
        for c in loads[:3]:
            c.wait()
    def prepare(j):
        with jax.named_scope("build"):
            build_dense(j, counts_ref, cols_ref, tiles_ref, at_ref)
        if j == 0:
            with jax.named_scope("wait_barrier"):
                pl.semaphore_wait(
                    barrier, n_col + flag(z < n_z - 1) + flag(z > 0) + flag(skips) + flag(from_skip)
                    + (flag(owner) + flag(apart) + PAIR * flag(inner) if owners else 0)
                )
        for p in range(2 * j, 2 * j + 2):
            at = p % 2 * rows
            for dy in range(1, n_y):
                to = (row, col_of(lax.rem(y + n_y - dy, n_y), k))
                if p < PIECES - 1:
                    q = p * plan.others + dy - 1
                    copy(at_ref.at[j, pl.ds(at, rows)], at_ref.at[plan.near + q, pl.ds(0, rows)],
                         a_send.at[0], a_recv.at[BC_DEV + 2 * q], to).start()
                    continue
                for h in range(CUTS):
                    t = h * plan.others + dy - 1
                    copy(at_ref.at[j, pl.ds(at + h * cut, cut)], tail_ref.at[t, pl.ds(0, cut)],
                         a_send.at[0], a_recv.at[BC_DEV + 2 * (plan.pairs + t)], to).start()
        copy(at_ref.at[j], at_ref.at[BC_DEV + j], a_send.at[0], a_recv.at[j], partner).start()

    prepare(0)

    def first(ref, at, size):
        return ref.at[at] if size == rows else ref.at[(*at, pl.ds(0, size))]

    def send(src, i, dst, at, size, send_sem, recv_sem, device):
        copy(first(src[0], (i,), size), first(dst[0], at, size), send_sem, recv_sem, device).start()
        copy(src[1].at[i], dst[1].at[at], send_sem, recv_sem, device).start()

    def taken(ref, at, size, recv_sem):
        both = size_ref if size == rows else small_ref
        pltpu.make_async_copy(both, both, recv_sem).wait()
        return decode(first(ref[0], at, size), ref[1].at[at])

    def send_x(i, value, kind=0):
        size = value.shape[0]
        encode(value, first(xs[0], (i,), size), xs[1].at[i])
        send(xs, i, xr, (i,), size, x_send.at[kind], x_recv.at[i], beside)

    def code_z(u, value):
        encode(value, first(zs[0], (u,), value.shape[0]), zs[1].at[u])

    def send_z(u, value):
        code_z(u, value)
        send(zs, u, zr, (to_side, u), value.shape[0], z_send.at[0], z_recv.at[to_side, u], onward)

    def send_part(u, value, which):
        code_z(u, value)
        send(zs, u, part, (which, u - plan.large), small, z_send.at[0], p_recv.at[which, u - plan.large], inner_of)

    def from_part(which, u):
        with jax.named_scope("wait_p"):
            return taken(part, (which, u - plan.large), small, p_recv.at[which, u - plan.large])

    def from_x(i, size):
        with jax.named_scope("wait_x"):
            return taken(xr, (i,), size, x_recv.at[i])

    def from_z(side, u, size):
        with jax.named_scope("wait_z"):
            return taken(zr, (side, u), size, z_recv.at[side, u])

    def dot(lhs, b_ref):
        return jnp.dot(lhs, b_ref[...], preferred_element_type=jnp.float32)

    def arrival(ref, n):
        copy(ref, ref, fw_send.at[0], a_recv.at[n], partner).wait_recv()

    def forward(ref, n, size):
        first, second = ref.at[pl.ds(0, size)], ref.at[pl.ds(size, size)]
        with jax.named_scope("wait_a"):
            arrival(first, n)
        copy(first, second, fw_send.at[0], a_recv.at[n + 1], partner).start()

    def forwarded(ref, n, size):
        with jax.named_scope("wait_f"):
            arrival(ref.at[pl.ds(size, size)], n + 1)

    def compute(d):
        @pl.when((d >= BC_DEV) & (d < plan.near))
        def _():
            arrival(at_ref.at[d], d - BC_DEV)

        @pl.when(d >= plan.near)
        def _():
            forwarded(at_ref.at[d], BC_DEV + 2 * (d - plan.near), rows)

        lhs = at_ref[d]
        with jax.named_scope("dot_away"):
            away = dot(lhs, b_away)
            for t in range(2):
                send_x(2 * d + t, away[t * rows : (t + 1) * rows])
        with jax.named_scope("dot_own"):
            own = dot(lhs, b_own)
            for t in range(2):
                own_ref[2 * d + t] = own[t * rows : (t + 1) * rows]

    def forward_tail(t):
        forward(tail_ref.at[t], BC_DEV + 2 * (plan.pairs + t), cut)

    def tail_away(t):
        n, i = BC_DEV + 2 * (plan.pairs + t), 2 * plan.slots + t

        @pl.when(t + 1 < plan.tails)
        def _():
            forward_tail(t + 1)

        forwarded(tail_ref.at[t], n, cut)
        with jax.named_scope("tail_away"):
            send_x(i, dot(tail_ref[t], b_away))

    def tail_own(g):
        both = tail_ref[pl.ds(2 * g, 2)].reshape(2 * small, tail_ref.shape[2])
        with jax.named_scope("tail_own"):
            own = dot(both, b_own)
            for t in range(2):
                own_ref[2 * plan.slots + 2 * g + t, pl.ds(0, small)] = own[t * small : (t + 1) * small]

    def work(s):
        @pl.when((lax.rem(s, 2) == 0) & (s < 2 * plan.slots))
        def _():
            compute(s // 2)

        @pl.when((lax.rem(s, 2) == 1) & (s >= 2 * plan.near - 1) & (s < 2 * plan.slots - 1))
        def _():
            d = (s + 1) // 2
            forward(at_ref.at[d], BC_DEV + 2 * (d - plan.near), rows)

        m = s - (2 * plan.slots - 1)

        @pl.when(m == 0)
        def _():
            forward_tail(0)
            tail_away(0)

        @pl.when((m >= 1) & (2 * m <= plan.tails))
        def _():
            tail_away(2 * m - 1)
            tail_own(m - 1)

        @pl.when((m >= 1) & (2 * m < plan.tails))
        def _():
            tail_away(2 * m)

    def fin_send(i, tail):
        def go(src, to_y, to_k, piece, at, size, sem):
            copy(src, land_ref.at[piece, pl.ds(at, size)], f_send.at[0], f_recv.at[sem],
                 (owner_row if tail and owners else row, col_of(to_y, to_k))).start()

        def cuts(h, src, at, to_y, to_k):
            go(src.at[i, pl.ds(at, cut)], to_y, to_k, PIECES - 1, h * cut, cut, PIECES - 1 + h)

        if tail:
            t = i - 2 * plan.slots
            h, dy = t // plan.others, lax.rem(t, plan.others) + 1
            for odd in range(2):
                cuts(h, fin_ref, odd * cut, lax.rem(y + dy, n_y), lax.rem(k + odd, PAIR))
            return

        @pl.when((i >= PIECES) & (i < 2 * PIECES - 1))
        def _():
            go(fin_ref.at[i], y, 1 - k, i - PIECES, 0, rows, i - PIECES)

        @pl.when(i == 2 * PIECES - 1)
        def _():
            for h in range(CUTS):
                cuts(h, fin_ref, h * cut, y, 1 - k)

        @pl.when(i >= 2 * PIECES)
        def _():
            q = i // 2 - plan.near
            p, dy = q // plan.others, lax.rem(q, plan.others) + 1
            go(fin_ref.at[i], lax.rem(y + dy, n_y), lax.rem(k + lax.rem(i, 2), PAIR), p, 0, rows, p)

    with jax.named_scope("wait_b"):
        loads[3].wait()
    with jax.named_scope("dot_first"):
        away = dot(at_ref[0], b_away)
        away_ref[...] = away[rows:]
        pl.when(outer)(lambda: send_z(0, away_ref[...]))
        send_x(0, away[:rows])

    prepare(1)
    loads[4].wait()
    with jax.named_scope("dot_first_own"):
        own = dot(at_ref[0], b_own)
        own_ref[0] = own[:rows]
        own_ref[1] = own[rows:]

        @pl.when(outer)
        def _():
            send_z(1, own_ref[1])

    def loop(lag, early, combine, late=0):
        def body(s, carry):
            work(s)
            e = s - lag
            if early is not None:
                pl.when(e == 0)(lambda: early(0))
                pl.when(e == 1)(lambda: early(1))

            tails_at = plan.large - late
            tail = (e >= tails_at) & (e < tails_at + plan.tails)

            @pl.when((e >= 2) & (e < plan.hops) & jnp.logical_not(tail))
            def _():
                u = jnp.where(e < tails_at, e, e - plan.tails)
                combine(u, jnp.where(u == 2, 0, u - 1), rows, False)

            @pl.when(tail)
            def _():
                combine(e + late, e + late - 1, small, True)

            return carry

        lax.fori_loop(2, plan.hops + lag, body, 0)

    def own(i, size):
        return first(own_ref, (i,), size)[...]

    @pl.when(outer)
    def _():
        def combine(u, i, size, tail):
            total = own(i, size) + from_x(i, size)
            if not (tail and owners):
                send_z(u, total)
                return
            pl.when(near)(lambda: send_part(u, total, 0))
            pl.when(jnp.logical_not(near))(lambda: send_z(u, total))

        loop(LAG_OUTER, None, combine)

    @pl.when(inner)
    def _():
        def early(u):
            send_z(u, (own_ref[1] if u else away_ref[...]) + from_z(from_side, u, rows))

        def combine(u, i, size, tail):
            total = own(i, size) + from_x(i, size) + from_z(from_side, u, size)
            if not (tail and owners):
                send_z(u, total)
                return
            total += from_part(0, u) + from_part(1, u)
            first(fin_ref, (i,), size)[...] = total.astype(jnp.bfloat16)
            fin_send(i, tail)

        loop(LAG_INNER, early, combine)

    @pl.when(final)
    def _():
        def early(u):
            total = (own_ref[1] if u else away_ref[...]) + from_z(0, u, rows) + from_z(1, u, rows)
            if u:
                own_ref[1] = total
            else:
                send_x(1, total, 1)

        def combine(u, i, size, tail):
            total = own(i, size) + from_x(i, size)
            if tail and owners:
                send_part(u, total, 1)
                return
            total += from_z(0, u, size) + from_z(1, u, size)
            first(fin_ref, (i,), size)[...] = total.astype(jnp.bfloat16)
            fin_send(i, tail)

            if not tail:
                @pl.when(u == 2 + Z_WAIT)
                def _():
                    fin_ref[1] = (own_ref[1] + from_x(1, rows)).astype(jnp.bfloat16)

        loop(LAG_FINAL, early, combine, LATE if owners else 0)

    def out(src, p, at, size):
        here = pl.ds(at, size)
        return pltpu.make_async_copy(src.at[p, here], o_ref.at[p, here], out_sem.at[0])

    def hand_over(p, at, size, sem):
        @pl.when(final)
        def _():
            out(fin_ref, p, at, size).start()

        @pl.when(jnp.logical_not(final))
        def _():
            here = land_ref.at[p, pl.ds(at, size)]
            with jax.named_scope("wait_land"):
                copy(here, here, f_send.at[0], f_recv.at[sem], partner).wait_recv()
            out(land_ref, p, at, size).start()

    def hand_over_cuts():
        for h in range(CUTS):
            hand_over(PIECES - 1, h * cut, cut, PIECES - 1 + h)

    for p in range(PIECES - 1):
        hand_over(p, 0, rows, p)
    hand_over_cuts()

    def drained(ref, sem, t=0):
        pltpu.make_async_copy(ref, ref, sem.at[t]).wait()

    with jax.named_scope("drain"):
        drained(at_ref.at[pl.ds(0, n_y * BC_DEV)], a_send)
        drained(at_ref.at[pl.ds(0, plan.others * BC_DEV)], fw_send)
        drained(x_size_ref, x_send)

        if owners:
            pl.when(outer)(lambda: drained(z_size_ref, z_send))
            pl.when(final)(lambda: drained(parts_size_ref, z_send))

            @pl.when(inner)
            def _():
                drained(large_size_ref, z_send)
                drained(fin_ref.at[pl.ds(0, plan.tails * small // rows)], f_send)
        else:
            pl.when(jnp.logical_not(final))(lambda: drained(z_size_ref, z_send))

        @pl.when(final)
        def _():
            drained(size_ref, x_send, 1)
            sent = 2 * plan.slots if owners else PIECES * n_col
            drained(fin_ref.at[pl.ds(PIECES, sent - PIECES)], f_send)

    with jax.named_scope("wait_out"):
        drained(o_ref, out_sem)


def per_device(n_row, n_col, tile_values, tile_counts, tile_cols, panels):
    slots, tile, _ = tile_values.shape
    deep, columns = panels.shape
    wide = columns // PAIR
    plan = Plan(n_col // PAIR)
    rows = BC_DEV * tile // PIECES
    f32, bf16, i16 = jnp.float32, jnp.bfloat16, jnp.int16
    hbm = pl.BlockSpec(memory_space=pl.ANY)
    dma = pltpu.SemaphoreType.DMA

    def coded(*lead):
        return pltpu.VMEM((*lead, rows, wide), i16), pltpu.VMEM((*lead, 1, wide), f32)

    def words(large, small):
        return pltpu.VMEM((1, (large * (rows // 2 + 1) + small * (rows // CUTS + 1)) * wide), f32)

    out = pl.pallas_call(
        functools.partial(kernel, n_row, n_col),
        out_shape=pltpu.VMEM((PIECES, rows, wide), bf16),
        in_specs=[hbm] * 4,
        out_specs=pl.BlockSpec(memory_space=pltpu.VMEM),
        scratch_shapes=[
            pltpu.SMEM(tile_counts.shape[::-1], jnp.int32),
            pltpu.SMEM(tile_cols.shape[::-1], jnp.int32),
            pltpu.VMEM((slots, tile, tile), bf16),
            pltpu.VMEM((deep, wide), bf16),
            pltpu.VMEM((deep, wide), bf16),
            pltpu.VMEM((plan.slots, 2 * rows, deep), bf16),
            pltpu.VMEM((plan.tails, 2 * rows // CUTS, deep), bf16),
            pltpu.VMEM((plan.units, rows, wide), f32),
            pltpu.VMEM((rows, wide), f32),
            coded(plan.units),
            coded(plan.units),
            coded(plan.hops),
            coded(2, plan.hops),
            coded(2, plan.tails),
            pltpu.VMEM((plan.units, rows, wide), bf16),
            pltpu.VMEM((PIECES, rows, wide), bf16),
            words(1, 0),
            words(0, 1),
            words(plan.large - 2, plan.tails),
            words(plan.large, plan.tails),
            words(plan.large, 0),
            words(0, plan.tails),
            dma((5,)),
            dma((1,)),
            dma((plan.arrivals,)),
            dma((1,)),
            dma((2,)),
            dma((plan.units,)),
            dma((1,)),
            dma((2, plan.hops)),
            dma((2, plan.tails)),
            dma((1,)),
            dma((PIECES - 1 + CUTS,)),
            dma((1,)),
        ],
        compiler_params=pltpu.CompilerParams(
            collective_id=0, has_side_effects=True, vmem_limit_bytes=56 * 1024 * 1024
        ),
    )(tile_counts.T, tile_cols.T, tile_values, panels)
    return out.reshape(BC_DEV * tile, wide)


def solution(mesh):
    n_row, n_col = mesh.shape["row"], mesh.shape["col"]
    return jax.shard_map(
        functools.partial(per_device, n_row, n_col),
        mesh=mesh,
        in_specs=(P("row", "col", None), P("row", "col"), P("row", "col"), P("row", "col")),
        out_specs=P("col", "row"),
        check_vma=False,
    )
```

```python
import functools

import jax
import jax.numpy as jnp
from jax import lax
from jax.experimental import pallas as pl
from jax.experimental.pallas import tpu as pltpu
from jax.sharding import PartitionSpec as P

BC_DEV = 2
PAIR = 2
PIECES = 4
CUTS = 4
Z_WAIT = 4
LATE = 4
LAG_OUTER = 1
LAG_INNER = 3
LAG_FINAL = 7
TOP = 32767.0
MESH = pl.DeviceIdType.MESH


class Plan:
    def __init__(self, n_y):
        self.others = n_y - 1
        self.near = 2 * BC_DEV
        self.pairs = (PIECES - 1) * self.others
        self.tails = CUTS * self.others
        self.slots = self.near + self.pairs
        self.units = 2 * self.slots + self.tails
        self.hops = self.units + 1
        self.large = self.hops - self.tails
        self.arrivals = BC_DEV + 2 * (self.pairs + self.tails)


def encode(value, code_ref, step_ref):
    peak = jnp.maximum(jnp.max(jnp.abs(value), axis=0, keepdims=True), 1e-30)
    code_ref[...] = jnp.round(value * (TOP / peak)).astype(jnp.int32).astype(jnp.int16)
    step_ref[...] = peak * (1.0 / TOP)


def decode(code_ref, step_ref):
    return code_ref[...].astype(jnp.int32).astype(jnp.float32) * step_ref[...]


def build_dense(j, counts_ref, cols_ref, tiles_ref, at_ref):
    slots, tile, _ = tiles_ref.shape
    start = jnp.int32(0)
    for i in range(counts_ref.shape[1]):
        count = counts_ref[0, i]
        here = jnp.minimum(start, slots - 1)
        after = jnp.minimum(start + 1, slots - 1)
        one = (count > 0) & (cols_ref[0, here] == j)
        two = (count > 1) & (cols_ref[0, after] == j)
        block = tiles_ref[jnp.where(two, after, here)]
        keep = jnp.where(one | two, 1.0, 0.0).astype(jnp.float32)
        at_ref[j, :, i * tile : (i + 1) * tile] = (block.astype(jnp.float32) * keep).T.astype(jnp.bfloat16)
        start = start + count


def kernel(
    n_row, n_col, counts_hbm, cols_hbm, tiles_hbm, b_hbm, o_ref,
    counts_ref, cols_ref, tiles_ref, b_away, b_own, at_ref, tail_ref, own_ref, away_ref, xs, xr, zs, zr, part,
    fin_ref, land_ref, size_ref, small_ref, x_size_ref, z_size_ref, large_size_ref,
    parts_size_ref, load_sem,
    a_send, a_recv, fw_send, x_send, x_recv, z_send, z_recv, p_recv, f_send, f_recv, out_sem,
):
    row, col = lax.axis_index("row"), lax.axis_index("col")
    n_z, n_y = n_row // PAIR, n_col // PAIR
    plan = Plan(n_y)
    z, x = row // PAIR, lax.rem(row, PAIR)
    y, k = col // PAIR, lax.rem(col, PAIR)
    wide = b_own.shape[1]
    rows = own_ref.shape[1]
    cut = rows // CUTS
    small = 2 * cut

    def row_of(z_at, x_at):
        return z_at * PAIR + x_at

    def col_of(y_at, k_at):
        return y_at * PAIR + k_at

    def load(src, dst, i):
        return pltpu.make_async_copy(src, dst, load_sem.at[i])

    at_away = pl.ds(pl.multiple_of((1 - x) * wide, wide), wide)
    at_own = pl.ds(pl.multiple_of(x * wide, wide), wide)
    loads = [
        load(tiles_hbm, tiles_ref, 0),
        load(counts_hbm, counts_ref, 3),
        load(cols_hbm, cols_ref, 4),
        load(b_hbm.at[:, at_away], b_away, 1),
        load(b_hbm.at[:, at_own], b_own, 2),
    ]
    for c in loads:
        c.start()

    beside = (row_of(z, 1 - x), col)
    partner = (row, col_of(y, 1 - k))
    final = z == col
    skip_up = (col == 0) & (z == 2)
    skip_dn = (col == n_z - 1) & (z == n_z - 3)
    low_end, high_end = (z == 0) & (col == 0), (z == n_z - 1) & (col == n_z - 1)
    skips, from_skip = skip_up | skip_dn, low_end | high_end
    from_above = (z > col) & (z < n_z - 1) & jnp.logical_not((col == 0) & (z == 1))
    from_below = (z < col) & (z > 0) & jnp.logical_not((col == n_z - 1) & (z == n_z - 2))
    inner = from_above | from_below
    outer = jnp.logical_not(final | inner)
    from_side = jnp.where(z > col, 0, 1)
    to_side = jnp.where(skips, 1 - from_side, from_side)
    z_next = jnp.where(final, jnp.where(z < n_z - 1, z + 1, z - 1), jnp.where(z > col, z - 1, z + 1))
    z_next = jnp.where(skips, jnp.minimum(col, n_z - 1), z_next)
    onward = (row_of(z_next, x), col)
    above = (row_of(jnp.minimum(z + 1, n_z - 1), x), col)
    below = (row_of(jnp.maximum(z - 1, 0), x), col)
    skip_of = (row_of(jnp.where(low_end, 2, n_z - 3), x), col)

    owners = n_z == 4 and n_y == 2
    owner = owners & (z // 2 != y)
    near = outer & (z // 2 == y)
    owner_row = row_of(jnp.minimum(col, n_z - 1), x)
    bringer = (row_of(jnp.where(z < 2, 2, 1), x), jnp.minimum(z, n_col - 1))
    inner_of = (row_of(jnp.where(y == 0, 2, 1), x), col)
    apart = (col == 1) & ((z == 0) | (z == 2)) | (col == 2) & ((z == 3) | (z == 1))
    apart_from = (row_of(jnp.clip(2 * col - z, 0, n_z - 1), x), col)

    def flag(b):
        return jnp.where(b, 1, 0).astype(jnp.int32)

    barrier = pltpu.get_barrier_semaphore()

    def greet(device):
        pl.semaphore_signal(barrier, inc=1, device_id=device, device_id_type=MESH)

    greet(beside)
    for step in range(1, n_col):
        greet((row, lax.rem(col + step, n_col)))
    pl.when(z < n_z - 1)(lambda: greet(above))
    pl.when(z > 0)(lambda: greet(below))
    pl.when(skips)(lambda: greet(onward))
    pl.when(from_skip)(lambda: greet(skip_of))
    if owners:
        pl.when(owner)(lambda: greet(bringer))
        pl.when(apart)(lambda: greet(apart_from))
        for k_at in range(PAIR):
            pl.when(inner)(lambda k_at=k_at: greet((owner_row, col_of(1 - y, k_at))))

    def copy(src, dst, send, recv, device):
        return pltpu.make_async_remote_copy(
            src_ref=src, dst_ref=dst, send_sem=send, recv_sem=recv,
            device_id=device, device_id_type=MESH,
        )

    with jax.named_scope("wait_tiles"):
        for c in loads[:3]:
            c.wait()
    def prepare(j):
        with jax.named_scope("build"):
            build_dense(j, counts_ref, cols_ref, tiles_ref, at_ref)
        if j == 0:
            with jax.named_scope("wait_barrier"):
                pl.semaphore_wait(
                    barrier, n_col + flag(z < n_z - 1) + flag(z > 0) + flag(skips) + flag(from_skip)
                    + (flag(owner) + flag(apart) + PAIR * flag(inner) if owners else 0)
                )
        for p in range(2 * j, 2 * j + 2):
            at = p % 2 * rows
            for dy in range(1, n_y):
                to = (row, col_of(lax.rem(y + n_y - dy, n_y), k))
                if p < PIECES - 1:
                    q = p * plan.others + dy - 1
                    copy(at_ref.at[j, pl.ds(at, rows)], at_ref.at[plan.near + q, pl.ds(0, rows)],
                         a_send.at[0], a_recv.at[BC_DEV + 2 * q], to).start()
                    continue
                for h in range(CUTS):
                    t = h * plan.others + dy - 1
                    copy(at_ref.at[j, pl.ds(at + h * cut, cut)], tail_ref.at[t, pl.ds(0, cut)],
                         a_send.at[0], a_recv.at[BC_DEV + 2 * (plan.pairs + t)], to).start()
        copy(at_ref.at[j], at_ref.at[BC_DEV + j], a_send.at[0], a_recv.at[j], partner).start()

    prepare(0)

    def first(ref, at, size):
        return ref.at[at] if size == rows else ref.at[(*at, pl.ds(0, size))]

    def send(src, i, dst, at, size, send_sem, recv_sem, device):
        copy(first(src[0], (i,), size), first(dst[0], at, size), send_sem, recv_sem, device).start()
        copy(src[1].at[i], dst[1].at[at], send_sem, recv_sem, device).start()

    def taken(ref, at, size, recv_sem):
        both = size_ref if size == rows else small_ref
        pltpu.make_async_copy(both, both, recv_sem).wait()
        return decode(first(ref[0], at, size), ref[1].at[at])

    def send_x(i, value, kind=0):
        size = value.shape[0]
        encode(value, first(xs[0], (i,), size), xs[1].at[i])
        send(xs, i, xr, (i,), size, x_send.at[kind], x_recv.at[i], beside)

    def code_z(u, value):
        encode(value, first(zs[0], (u,), value.shape[0]), zs[1].at[u])

    def send_z(u, value):
        code_z(u, value)
        send(zs, u, zr, (to_side, u), value.shape[0], z_send.at[0], z_recv.at[to_side, u], onward)

    def send_part(u, value, which):
        code_z(u, value)
        send(zs, u, part, (which, u - plan.large), small, z_send.at[0], p_recv.at[which, u - plan.large], inner_of)

    def from_part(which, u):
        with jax.named_scope("wait_p"):
            return taken(part, (which, u - plan.large), small, p_recv.at[which, u - plan.large])

    def from_x(i, size):
        with jax.named_scope("wait_x"):
            return taken(xr, (i,), size, x_recv.at[i])

    def from_z(side, u, size):
        with jax.named_scope("wait_z"):
            return taken(zr, (side, u), size, z_recv.at[side, u])

    def dot(lhs, b_ref):
        return jnp.dot(lhs, b_ref[...], preferred_element_type=jnp.float32)

    def arrival(ref, n):
        copy(ref, ref, fw_send.at[0], a_recv.at[n], partner).wait_recv()

    def forward(ref, n, size):
        first, second = ref.at[pl.ds(0, size)], ref.at[pl.ds(size, size)]
        with jax.named_scope("wait_a"):
            arrival(first, n)
        copy(first, second, fw_send.at[0], a_recv.at[n + 1], partner).start()

    def forwarded(ref, n, size):
        with jax.named_scope("wait_f"):
            arrival(ref.at[pl.ds(size, size)], n + 1)

    def compute(d):
        @pl.when((d >= BC_DEV) & (d < plan.near))
        def _():
            arrival(at_ref.at[d], d - BC_DEV)

        @pl.when(d >= plan.near)
        def _():
            forwarded(at_ref.at[d], BC_DEV + 2 * (d - plan.near), rows)

        lhs = at_ref[d]
        with jax.named_scope("dot_away"):
            away = dot(lhs, b_away)
            for t in range(2):
                send_x(2 * d + t, away[t * rows : (t + 1) * rows])
        with jax.named_scope("dot_own"):
            own = dot(lhs, b_own)
            for t in range(2):
                own_ref[2 * d + t] = own[t * rows : (t + 1) * rows]

    def forward_tail(t):
        forward(tail_ref.at[t], BC_DEV + 2 * (plan.pairs + t), cut)

    def tail_away(t):
        n, i = BC_DEV + 2 * (plan.pairs + t), 2 * plan.slots + t

        @pl.when(t + 1 < plan.tails)
        def _():
            forward_tail(t + 1)

        forwarded(tail_ref.at[t], n, cut)
        with jax.named_scope("tail_away"):
            send_x(i, dot(tail_ref[t], b_away))

    def tail_own(g):
        both = tail_ref[pl.ds(2 * g, 2)].reshape(2 * small, tail_ref.shape[2])
        with jax.named_scope("tail_own"):
            own = dot(both, b_own)
            for t in range(2):
                own_ref[2 * plan.slots + 2 * g + t, pl.ds(0, small)] = own[t * small : (t + 1) * small]

    def work(s):
        @pl.when((lax.rem(s, 2) == 0) & (s < 2 * plan.slots))
        def _():
            compute(s // 2)

        @pl.when((lax.rem(s, 2) == 1) & (s >= 2 * plan.near - 1) & (s < 2 * plan.slots - 1))
        def _():
            d = (s + 1) // 2
            forward(at_ref.at[d], BC_DEV + 2 * (d - plan.near), rows)

        m = s - (2 * plan.slots - 1)

        @pl.when(m == 0)
        def _():
            forward_tail(0)
            tail_away(0)

        @pl.when((m >= 1) & (2 * m <= plan.tails))
        def _():
            tail_away(2 * m - 1)
            tail_own(m - 1)

        @pl.when((m >= 1) & (2 * m < plan.tails))
        def _():
            tail_away(2 * m)

    def fin_send(i, tail):
        def go(src, to_y, to_k, piece, at, size, sem):
            copy(src, land_ref.at[piece, pl.ds(at, size)], f_send.at[0], f_recv.at[sem],
                 (owner_row if tail and owners else row, col_of(to_y, to_k))).start()

        def cuts(h, src, at, to_y, to_k):
            go(src.at[i, pl.ds(at, cut)], to_y, to_k, PIECES - 1, h * cut, cut, PIECES - 1 + h)

        if tail:
            t = i - 2 * plan.slots
            h, dy = t // plan.others, lax.rem(t, plan.others) + 1
            for odd in range(2):
                cuts(h, fin_ref, odd * cut, lax.rem(y + dy, n_y), lax.rem(k + odd, PAIR))
            return

        @pl.when((i >= PIECES) & (i < 2 * PIECES - 1))
        def _():
            go(fin_ref.at[i], y, 1 - k, i - PIECES, 0, rows, i - PIECES)

        @pl.when(i == 2 * PIECES - 1)
        def _():
            for h in range(CUTS):
                cuts(h, fin_ref, h * cut, y, 1 - k)

        @pl.when(i >= 2 * PIECES)
        def _():
            q = i // 2 - plan.near
            p, dy = q // plan.others, lax.rem(q, plan.others) + 1
            go(fin_ref.at[i], lax.rem(y + dy, n_y), lax.rem(k + lax.rem(i, 2), PAIR), p, 0, rows, p)

    with jax.named_scope("wait_b"):
        loads[3].wait()
    with jax.named_scope("dot_first"):
        away = dot(at_ref[0], b_away)
        away_ref[...] = away[rows:]
        pl.when(outer)(lambda: send_z(0, away_ref[...]))
        send_x(0, away[:rows])

    prepare(1)
    loads[4].wait()
    with jax.named_scope("dot_first_own"):
        own = dot(at_ref[0], b_own)
        own_ref[0] = own[:rows]
        own_ref[1] = own[rows:]

        @pl.when(outer)
        def _():
            send_z(1, own_ref[1])

    def loop(lag, early, combine, late=0):
        def body(s, carry):
            work(s)
            e = s - lag
            if early is not None:
                pl.when(e == 0)(lambda: early(0))
                pl.when(e == 1)(lambda: early(1))

            tails_at = plan.large - late
            tail = (e >= tails_at) & (e < tails_at + plan.tails)

            @pl.when((e >= 2) & (e < plan.hops) & jnp.logical_not(tail))
            def _():
                u = jnp.where(e < tails_at, e, e - plan.tails)
                combine(u, jnp.where(u == 2, 0, u - 1), rows, False)

            @pl.when(tail)
            def _():
                combine(e + late, e + late - 1, small, True)

            return carry

        lax.fori_loop(2, plan.hops + lag, body, 0)

    def own(i, size):
        return first(own_ref, (i,), size)[...]

    @pl.when(outer)
    def _():
        def combine(u, i, size, tail):
            total = own(i, size) + from_x(i, size)
            if not (tail and owners):
                send_z(u, total)
                return
            pl.when(near)(lambda: send_part(u, total, 0))
            pl.when(jnp.logical_not(near))(lambda: send_z(u, total))

        loop(LAG_OUTER, None, combine)

    @pl.when(inner)
    def _():
        def early(u):
            send_z(u, (own_ref[1] if u else away_ref[...]) + from_z(from_side, u, rows))

        def combine(u, i, size, tail):
            total = own(i, size) + from_x(i, size) + from_z(from_side, u, size)
            if not (tail and owners):
                send_z(u, total)
                return
            total += from_part(0, u) + from_part(1, u)
            first(fin_ref, (i,), size)[...] = total.astype(jnp.bfloat16)
            fin_send(i, tail)

        loop(LAG_INNER, early, combine)

    @pl.when(final)
    def _():
        def early(u):
            total = (own_ref[1] if u else away_ref[...]) + from_z(0, u, rows) + from_z(1, u, rows)
            if u:
                own_ref[1] = total
            else:
                send_x(1, total, 1)

        def combine(u, i, size, tail):
            total = own(i, size) + from_x(i, size)
            if tail and owners:
                send_part(u, total, 1)
                return
            total += from_z(0, u, size) + from_z(1, u, size)
            first(fin_ref, (i,), size)[...] = total.astype(jnp.bfloat16)
            fin_send(i, tail)

            if not tail:
                @pl.when(u == 2 + Z_WAIT)
                def _():
                    fin_ref[1] = (own_ref[1] + from_x(1, rows)).astype(jnp.bfloat16)

        loop(LAG_FINAL, early, combine, LATE if owners else 0)

    def out(src, p, at, size):
        here = pl.ds(at, size)
        return pltpu.make_async_copy(src.at[p, here], o_ref.at[p, here], out_sem.at[0])

    def hand_over(p, at, size, sem):
        @pl.when(final)
        def _():
            out(fin_ref, p, at, size).start()

        @pl.when(jnp.logical_not(final))
        def _():
            here = land_ref.at[p, pl.ds(at, size)]
            with jax.named_scope("wait_land"):
                copy(here, here, f_send.at[0], f_recv.at[sem], partner).wait_recv()
            out(land_ref, p, at, size).start()

    def hand_over_cuts():
        for h in range(CUTS):
            hand_over(PIECES - 1, h * cut, cut, PIECES - 1 + h)

    for p in range(PIECES - 1):
        hand_over(p, 0, rows, p)
    hand_over_cuts()

    def drained(ref, sem, t=0):
        pltpu.make_async_copy(ref, ref, sem.at[t]).wait()

    with jax.named_scope("drain"):
        drained(at_ref.at[pl.ds(0, n_y * BC_DEV)], a_send)
        drained(at_ref.at[pl.ds(0, plan.others * BC_DEV)], fw_send)
        drained(x_size_ref, x_send)

        if owners:
            pl.when(outer)(lambda: drained(z_size_ref, z_send))
            pl.when(final)(lambda: drained(parts_size_ref, z_send))

            @pl.when(inner)
            def _():
                drained(large_size_ref, z_send)
                drained(fin_ref.at[pl.ds(0, plan.tails * small // rows)], f_send)
        else:
            pl.when(jnp.logical_not(final))(lambda: drained(z_size_ref, z_send))

        @pl.when(final)
        def _():
            drained(size_ref, x_send, 1)
            sent = 2 * plan.slots if owners else PIECES * n_col
            drained(fin_ref.at[pl.ds(PIECES, sent - PIECES)], f_send)

    with jax.named_scope("wait_out"):
        drained(o_ref, out_sem)


def per_device(n_row, n_col, tile_values, tile_counts, tile_cols, panels):
    slots, tile, _ = tile_values.shape
    deep, columns = panels.shape
    wide = columns // PAIR
    plan = Plan(n_col // PAIR)
    rows = BC_DEV * tile // PIECES
    f32, bf16, i16 = jnp.float32, jnp.bfloat16, jnp.int16
    hbm = pl.BlockSpec(memory_space=pl.ANY)
    dma = pltpu.SemaphoreType.DMA

    def coded(*lead):
        return pltpu.VMEM((*lead, rows, wide), i16), pltpu.VMEM((*lead, 1, wide), f32)

    def words(large, small):
        return pltpu.VMEM((1, (large * (rows // 2 + 1) + small * (rows // CUTS + 1)) * wide), f32)

    out = pl.pallas_call(
        functools.partial(kernel, n_row, n_col),
        out_shape=pltpu.VMEM((PIECES, rows, wide), bf16),
        in_specs=[hbm] * 4,
        out_specs=pl.BlockSpec(memory_space=pltpu.VMEM),
        scratch_shapes=[
            pltpu.SMEM(tile_counts.shape[::-1], jnp.int32),
            pltpu.SMEM(tile_cols.shape[::-1], jnp.int32),
            pltpu.VMEM((slots, tile, tile), bf16),
            pltpu.VMEM((deep, wide), bf16),
            pltpu.VMEM((deep, wide), bf16),
            pltpu.VMEM((plan.slots, 2 * rows, deep), bf16),
            pltpu.VMEM((plan.tails, 2 * rows // CUTS, deep), bf16),
            pltpu.VMEM((plan.units, rows, wide), f32),
            pltpu.VMEM((rows, wide), f32),
            coded(plan.units),
            coded(plan.units),
            coded(plan.hops),
            coded(2, plan.hops),
            coded(2, plan.tails),
            pltpu.VMEM((plan.units, rows, wide), bf16),
            pltpu.VMEM((PIECES, rows, wide), bf16),
            words(1, 0),
            words(0, 1),
            words(plan.large - 2, plan.tails),
            words(plan.large, plan.tails),
            words(plan.large, 0),
            words(0, plan.tails),
            dma((5,)),
            dma((1,)),
            dma((plan.arrivals,)),
            dma((1,)),
            dma((2,)),
            dma((plan.units,)),
            dma((1,)),
            dma((2, plan.hops)),
            dma((2, plan.tails)),
            dma((1,)),
            dma((PIECES - 1 + CUTS,)),
            dma((1,)),
        ],
        compiler_params=pltpu.CompilerParams(
            collective_id=0, has_side_effects=True, vmem_limit_bytes=56 * 1024 * 1024
        ),
    )(tile_counts.T, tile_cols.T, tile_values, panels)
    return out.reshape(BC_DEV * tile, wide)


def solution(mesh):
    n_row, n_col = mesh.shape["row"], mesh.shape["col"]
    return jax.shard_map(
        functools.partial(per_device, n_row, n_col),
        mesh=mesh,
        in_specs=(P("row", "col", None), P("row", "col"), P("row", "col"), P("row", "col")),
        out_specs=P("col", "row"),
        check_vma=False,
    )
```
